32 devices in a mesh: dp: 2 (over x), sp: 16 (over y, z, core).
Axes of the slice: x: 2, y: 2, z: 4, core: 2. Of those that a mesh axis runs over, the one named last changes fastest.
Arguments:
- x: bfloat16 [16384, 2560], P(('dp', 'sp')), parts along dimension 0
- gain: bfloat16 [2560], replicated
- wq: bfloat16 [2560, 2048], P('sp')
- wk: bfloat16 [2560, 1024], P('sp')
- wv: bfloat16 [2560, 1024], P('sp')
- wo: bfloat16 [2048, 2560], P('sp')
Outputs:
- output: bfloat16 [16384, 2560], P(('dp', 'sp')), parts along dimension 0
There are 2 independent parts. The reference program is written for one: setup_inputs(seed, part) draws one part's arguments, and reference() takes and returns one part's arrays. A program takes and returns all parts, laid end to end along the dimension named above; an argument that names none is the same for every part.
All inputs are finite; a program needn't handle non-finite values.
Results may differ from the reference program's by a relative error of at most 0.012.
Values are sent between devices in bfloat16 or wider.
A program may use at most 2 GiB of HBM per device.

```python
import jax
import jax.numpy as jnp
from jax import lax

ROWS = 8192
D = 2560
HEADS = 8
KV_HEADS = 4
HEAD = 256
THETA = 10000


def setup_inputs(seed: int = 0, part: int = 0) -> dict:
    kx, kn, kq, kk, kv, ko = jax.random.split(jax.random.key(seed), 6)

    def weights(key, rows, columns):
        return jax.random.normal(key, (rows, columns), jnp.float32) * rows**-0.5

    drawn = {
        "x": jax.random.normal(jax.random.fold_in(kx, part), (ROWS, D), jnp.float32),
        "gain": 1 + 0.1 * jax.random.normal(kn, (D,), jnp.float32),
        "wq": 2 * weights(kq, D, HEADS * HEAD),
        "wk": 2 * weights(kk, D, KV_HEADS * HEAD),
        "wv": 4 * weights(kv, D, KV_HEADS * HEAD),
        "wo": weights(ko, HEADS * HEAD, D),
    }
    return {k: v.astype(jnp.bfloat16) for k, v in drawn.items()}


def normed(x, gain):
    wide = x.astype(jnp.float32)
    scale = lax.rsqrt(jnp.mean(wide * wide, -1, keepdims=True) + 1e-6)
    return (wide * scale * gain.astype(jnp.float32)).astype(jnp.bfloat16)


def turned(t, place, theta):
    half = t.shape[-1] // 2
    angle = place.astype(jnp.float32)[:, None] * theta ** (-jnp.arange(half, dtype=jnp.float32) / half)
    cos, sin = jnp.cos(angle)[:, None], jnp.sin(angle)[:, None]
    a, b = t[..., :half].astype(jnp.float32), t[..., half:].astype(jnp.float32)
    return jnp.concatenate([a * cos - b * sin, b * cos + a * sin], -1).astype(jnp.bfloat16)


def matmul(a, w):
    return jnp.dot(a, w, preferred_element_type=jnp.float32).astype(jnp.bfloat16)


def einsum(form, a, b):
    return jnp.einsum(form, a.astype(jnp.float32), b.astype(jnp.float32))


def attention(q, k, v):
    scores = einsum("tgsd,ugd->gstu", q, k) * q.shape[-1] ** -0.5
    token = jnp.arange(q.shape[0])
    scores = jnp.where(token[:, None] >= token, scores, -jnp.inf)
    weights = jax.nn.softmax(scores, -1).astype(jnp.bfloat16)
    return einsum("gstu,ugd->tgsd", weights, v).astype(jnp.bfloat16)


def reference(x, gain, wq, wk, wv, wo):
    a, place = normed(x, gain), jnp.arange(ROWS)
    q = turned(matmul(a, wq).reshape(ROWS, HEADS, HEAD), place, THETA).reshape(ROWS, KV_HEADS, -1, HEAD)
    k = turned(matmul(a, wk).reshape(ROWS, KV_HEADS, HEAD), place, THETA)
    v = matmul(a, wv).reshape(ROWS, KV_HEADS, HEAD)
    seen = attention(q, k, v).reshape(ROWS, HEADS * HEAD)
    return (x.astype(jnp.float32) + jnp.dot(seen, wo, preferred_element_type=jnp.float32)).astype(jnp.bfloat16)
```

```python
import functools

import jax
import jax.numpy as jnp
from jax import lax
from jax.experimental import pallas as pl
from jax.experimental.pallas import tpu as pltpu
from jax.sharding import PartitionSpec as P

NEG = -1e30
HIDDEN = 2 * NEG
LOG2E = 1.4426950408889634
VMEM = 56 * 2**20
HEAD = 256
THETA = 10000
MESH = pl.DeviceIdType.MESH


def normed(x, gain):
    wide = x.astype(jnp.float32)
    scale = lax.rsqrt(jnp.mean(wide * wide, -1, keepdims=True) + 1e-6)
    return (wide * scale * gain.astype(jnp.float32)).astype(jnp.bfloat16)


def turned(t, place, theta):
    half = t.shape[-1] // 2
    angle = place.astype(jnp.float32)[:, None] * theta ** (-jnp.arange(half, dtype=jnp.float32) / half)
    cos, sin = jnp.cos(angle)[:, None], jnp.sin(angle)[:, None]
    a, b = t[..., :half].astype(jnp.float32), t[..., half:].astype(jnp.float32)
    return jnp.concatenate([a * cos - b * sin, b * cos + a * sin], -1).astype(jnp.bfloat16)


def matmul(a, w):
    return jnp.dot(a, w, preferred_element_type=jnp.float32).astype(jnp.bfloat16)


def _dot(a, b, ca, cb):
    return lax.dot_general(a, b, (((ca,), (cb,)), ((), ())), preferred_element_type=jnp.float32)


def flip(s, k):
    for bit in (1, 2, 4, 8):
        if k & bit:
            s = s + bit - 2 * bit * lax.rem(lax.div(s, bit), 2)
    return s


def meet(s, d, ks, across):
    barrier = pltpu.get_barrier_semaphore()
    for k in ks:
        pl.semaphore_signal(barrier, inc=1, device_id={"sp": flip(s, k)}, device_id_type=MESH)
    if across:
        pl.semaphore_signal(barrier, inc=1, device_id={"dp": 1 - d}, device_id_type=MESH)
    pl.semaphore_wait(barrier, len(ks) + across)


ROWS = 4


def gather(a_ref, w_ref, o_ref, aa_ref, ww_ref, oo_ref, local, ws, wr, xs, xr, as_, ar, fs, fr, os_, or_, oxs, oxr, ods, odr):
    s, d = lax.axis_index("sp"), lax.axis_index("dp")
    g = lax.rem(s, 4)
    meet(s, d, (1, 2, 3, 4, 8), True)
    sends = []

    def send(src, dst, ssem, rsem, to):
        copy = pltpu.make_async_remote_copy(src_ref=src, dst_ref=dst, send_sem=ssem, recv_sem=rsem, device_id=to, device_id_type=MESH)
        copy.start()
        sends.append(copy)

    def arrived(dst, rsem):
        pltpu.make_async_copy(dst, dst, rsem).wait()

    def keep(src, dst, sem):
        copy = pltpu.make_async_copy(src, dst, sem)
        copy.start()
        return copy

    other = 1 - d
    for part in (d, other):
        for m in (2, 3, 1):
            send(w_ref.at[part, flip(g, m)], ww_ref.at[part, s], ws.at[part, m - 1], wr.at[part, m - 1], {"sp": flip(s, m)})
    kept = [keep(w_ref.at[p, g], ww_ref.at[p, s], local.at[p]) for p in (0, 1)]
    kept.append(keep(a_ref, aa_ref.at[g], local.at[2]))
    kept += [keep(o_ref.at[p], oo_ref.at[p, s], local.at[3 + p]) for p in (0, 1)]
    for k in (0, 1, 2, 3):
        at = flip(s, k)
        if k:
            arrived(ww_ref.at[d, at], wr.at[d, k - 1])
        src = ww_ref.at[d, at] if k else w_ref.at[d, g]
        send(src, ww_ref.at[d, at], ws.at[d, 3 + k], wr.at[d, 3 + k], {"sp": flip(s, 4)})
        send(src, ww_ref.at[d, at], ws.at[d, 7 + k], wr.at[d, 7 + k], {"sp": flip(s, 8)})
    n = a_ref.shape[0] // ROWS
    for i in range(ROWS):
        rows = pl.ds(i * n, n)
        send(a_ref.at[rows], aa_ref.at[g, rows], as_.at[0, i], ar.at[0, i], {"sp": flip(s, 2)})
        send(a_ref.at[rows], aa_ref.at[g, rows], as_.at[1, i], ar.at[1, i], {"sp": flip(s, 1)})
    send(o_ref.at[d], oo_ref.at[d, s], os_.at[0], or_.at[0], {"sp": flip(s, 2)})
    for k in range(4, 16):
        at = flip(s, k)
        arrived(ww_ref.at[d, at], wr.at[d, 3 + k - 4] if k < 8 else wr.at[d, 7 + k - 8])
        if k < 8:
            send(ww_ref.at[d, at], ww_ref.at[d, at], ws.at[d, 7 + k], wr.at[d, 7 + k], {"sp": flip(s, 8)})
        send(ww_ref.at[d, at], ww_ref.at[d, at], xs.at[k - 4], xr.at[k - 4], {"dp": other})
    for i in range(ROWS):
        rows = pl.ds(i * n, n)
        arrived(aa_ref.at[flip(g, 2), rows], ar.at[0, i])
        send(aa_ref.at[flip(g, 2), rows], aa_ref.at[flip(g, 2), rows], fs.at[i], fr.at[i], {"sp": flip(s, 1)})
    for i, k in enumerate((0, 2, 4, 6, 8, 10, 12, 14)):
        at = flip(s, k)
        src = oo_ref.at[d, at] if k else o_ref.at[d]
        if k:
            arrived(oo_ref.at[d, at], or_.at[i - 1])
        if k < 4:
            send(src, oo_ref.at[d, at], os_.at[1 + i], or_.at[1 + i], {"sp": flip(s, 4)})
        if k < 8:
            send(src, oo_ref.at[d, at], os_.at[3 + i], or_.at[3 + i], {"sp": flip(s, 8)})
        if k:
            send(src, oo_ref.at[d, at], oxs.at[i - 1], oxr.at[i - 1], {"dp": other})
        send(src, oo_ref.at[d, at], ods.at[0, i], odr.at[0, i], {"sp": flip(s, 1)})
    for i, k in enumerate((0, 2, 4, 6, 8, 10, 12, 14)):
        at = flip(s, k)
        src = oo_ref.at[other, at] if k else o_ref.at[other]
        if k:
            arrived(oo_ref.at[other, at], oxr.at[i - 1])
        send(src, oo_ref.at[other, at], ods.at[1, i], odr.at[1, i], {"sp": flip(s, 1)})
    for m in (1, 2, 3):
        arrived(ww_ref.at[other, flip(s, m)], wr.at[other, m - 1])
    for k in range(4, 16):
        arrived(ww_ref.at[other, flip(s, k)], xr.at[k - 4])
    for i in range(ROWS):
        rows = pl.ds(i * n, n)
        arrived(aa_ref.at[flip(g, 1), rows], ar.at[1, i])
        arrived(aa_ref.at[flip(g, 3), rows], fr.at[i])
    for i, k in enumerate((0, 2, 4, 6, 8, 10, 12, 14)):
        arrived(oo_ref.at[d, flip(s, k + 1)], odr.at[0, i])
        arrived(oo_ref.at[other, flip(s, k + 1)], odr.at[1, i])
    for copy in kept:
        copy.wait()
    for copy in sends:
        copy.wait_send()


def gathered(a, w, o):
    dma = pltpu.SemaphoreType.DMA
    vmem, hbm = pl.BlockSpec(memory_space=pltpu.VMEM), pl.BlockSpec(memory_space=pl.ANY)
    shape = lambda *n: jax.ShapeDtypeStruct(n, jnp.bfloat16)
    return pl.pallas_call(
        gather,
        out_shape=[shape(4, *a.shape), shape(2, 16, *w.shape[2:]), shape(2, 16, *o.shape[1:])],
        in_specs=[vmem] * 3,
        out_specs=[hbm] * 3,
        scratch_shapes=[dma((5,)), dma((2, 15)), dma((2, 15)), dma((12,)), dma((12,)), dma((2, ROWS)), dma((2, ROWS)), dma((ROWS,)), dma((ROWS,)),
                        dma((7,)), dma((7,)), dma((7,)), dma((7,)), dma((2, 8)), dma((2, 8))],
        compiler_params=pltpu.CompilerParams(collective_id=0, has_side_effects=True, vmem_limit_bytes=VMEM),
    )(a, w, o)


CHUNKS = 4
STRIP = 512


def attention(q_ref, kv_ref, seen_ref, got, top_s, mix_s, out_s, gap_s, send_sem, recv_sem, osend, orecv, local):
    s, d = lax.axis_index("sp"), lax.axis_index("dp")
    g, zh, y = lax.rem(s, 4), lax.rem(lax.div(s, 4), 2), lax.div(s, 8)
    tokens = kv_ref.shape[0]
    n = tokens // CHUNKS
    strips = tokens // STRIP
    pieces = [(i, h) for i in range(strips) for h in range(2)]
    e = HEAD**-0.5 * LOG2E
    meet(s, d, (1, 2, 3, 4, 8), False)

    def copy(src, kind, i, k):
        return pltpu.make_async_remote_copy(src_ref=src, dst_ref=got.at[kind, pl.ds(i * n, n)], send_sem=send_sem.at[kind, i],
                                            recv_sem=recv_sem.at[kind, i], device_id={"sp": flip(s, k)}, device_id_type=MESH)

    own = lambda i: kv_ref.at[pl.ds(i * n, n)]
    to_z = (y == 0) | (zh == 0)
    from_z = (y == 0) | (zh == 1)
    for i in range(CHUNKS):
        @pl.when(to_z)
        def _():
            copy(own(i), 1, i, 4).start()

        @pl.when(y == 0)
        def _():
            copy(own(i), 0, i, 8).start()

    top_s[...] = jnp.full(top_s.shape, NEG, jnp.float32)
    mix_s[...] = jnp.zeros(mix_s.shape, jnp.float32)
    gap_s[...] = lax.broadcasted_iota(jnp.int32, gap_s.shape, 1) - lax.broadcasted_iota(jnp.int32, gap_s.shape, 0)
    ones = jnp.ones((8, n), jnp.bfloat16)

    def block(keys, values, first):
        scores = [_dot(keys, q_ref[i * STRIP : (i + 1) * STRIP, h * HEAD : (h + 1) * HEAD], 1, 1) for i, h in pieces]
        weights, keeps = [], []
        for at, ((i, h), sc) in enumerate(zip(pieces, scores)):
            cols = slice(at * STRIP, (at + 1) * STRIP)
            if first is not None:
                sc = jnp.where(gap_s[...] >= first - i * STRIP, sc, HIDDEN)
            old = top_s[:, cols]
            top = jnp.maximum(old, sc.max(axis=0, keepdims=True))
            top_s[:, cols] = top
            weights.append(jnp.exp2((sc - top) * e).astype(jnp.bfloat16))
            keeps.append(jnp.exp2((old - top) * e))
        turned_values = jnp.concatenate([values.T, ones], axis=0)
        for at, (p, keep) in enumerate(zip(weights, keeps)):
            cols = slice(at * STRIP, (at + 1) * STRIP)
            mix_s[:, cols] = mix_s[:, cols] * keep + _dot(turned_values, p, 1, 0)

    def own_block(i, _):
        rows = pl.ds(pl.multiple_of(i * n, n), n)
        block(kv_ref[rows, :HEAD], kv_ref[rows, HEAD:], i * n)

    lax.fori_loop(0, CHUNKS, own_block, None)

    def step(t, _):
        kind, i = lax.div(t, CHUNKS), lax.rem(t, CHUNKS)
        rows = pl.ds(pl.multiple_of(i * n, n), n)
        comes = jnp.where(kind == 1, from_z, y == 1)
        wanted = jnp.where(kind == 1, zh == 1, y == 1)

        @pl.when(comes)
        def _():
            here = got.at[kind, rows]
            pltpu.make_async_copy(here, here, recv_sem.at[kind, i]).wait()

        @pl.when((kind == 1) & (y == 0))
        def _():
            pltpu.make_async_remote_copy(src_ref=got.at[1, rows], dst_ref=got.at[2, rows], send_sem=send_sem.at[2, i], recv_sem=recv_sem.at[2, i],
                                         device_id={"sp": flip(s, 8)}, device_id_type=MESH).start()

        @pl.when(wanted)
        def _():
            block(got[kind, rows, :HEAD], got[kind, rows, HEAD:], None)

    lax.fori_loop(0, 3 * CHUNKS, step, None)

    for at, (i, h) in enumerate(pieces):
        cols = slice(at * STRIP, (at + 1) * STRIP)
        out = mix_s[:HEAD, cols] * (1 / mix_s[HEAD : HEAD + 1, cols])
        out_s[i, :, h * HEAD : (h + 1) * HEAD] = out.T.astype(jnp.bfloat16)
    mine = pl.ds(pl.multiple_of(g * 2 * HEAD, 2 * HEAD), 2 * HEAD)
    back = []
    for m in (2, 3, 1):
        back.append(pltpu.make_async_remote_copy(src_ref=out_s.at[flip(g, m)], dst_ref=seen_ref.at[:, mine], send_sem=osend.at[m - 1],
                                                 recv_sem=orecv.at[m - 1], device_id={"sp": flip(s, m)}, device_id_type=MESH))
        back[-1].start()
    kept = pltpu.make_async_copy(out_s.at[g], seen_ref.at[:, mine], local)
    kept.start()
    for m in (1, 2, 3):
        here = seen_ref.at[:, pl.ds(pl.multiple_of(flip(g, m) * 2 * HEAD, 2 * HEAD), 2 * HEAD)]
        pltpu.make_async_copy(here, here, orecv.at[m - 1]).wait()
    kept.wait()
    for c in back:
        c.wait_send()
    for i in range(CHUNKS):
        @pl.when(to_z)
        def _():
            copy(own(i), 1, i, 4).wait_send()

        @pl.when(y == 0)
        def _():
            copy(own(i), 0, i, 8).wait_send()
            copy(own(i), 2, i, 8).wait_send()


def attended(q, kv, own):
    dma = pltpu.SemaphoreType.DMA
    tokens = q.shape[0]
    vmem = pl.BlockSpec(memory_space=pltpu.VMEM)
    return pl.pallas_call(
        attention,
        out_shape=jax.ShapeDtypeStruct((own, 4 * 2 * HEAD), jnp.bfloat16),
        in_specs=[vmem] * 2,
        out_specs=pl.BlockSpec(memory_space=pl.ANY),
        scratch_shapes=[
            pltpu.VMEM((3, tokens, 2 * HEAD), jnp.bfloat16),
            pltpu.VMEM((1, 2 * tokens), jnp.float32),
            pltpu.VMEM((HEAD + 8, 2 * tokens), jnp.float32),
            pltpu.VMEM((4, own, 2 * HEAD), jnp.bfloat16),
            pltpu.VMEM((tokens // CHUNKS, STRIP), jnp.int32),
            dma((3, CHUNKS)), dma((3, CHUNKS)), dma((3,)), dma((3,)), dma,
        ],
        compiler_params=pltpu.CompilerParams(collective_id=1, has_side_effects=True, vmem_limit_bytes=VMEM),
    )(q, kv)


def solution(mesh):
    def step(x, gain, wq, wk, wv, wo):
        own = x.shape[0]
        s = lax.axis_index("sp")
        a = normed(x, gain)
        r = wk.shape[0]
        wkv = jnp.concatenate([wk.reshape(r, 4, HEAD), wv.reshape(r, 4, HEAD)], -1)
        w = jnp.stack([wkv.transpose(1, 0, 2), wq.reshape(r, 4, 2 * HEAD).transpose(1, 0, 2)])
        o = wo.reshape(wo.shape[0], 2, -1).transpose(1, 0, 2)
        a, w, o = gathered(a, w, o)
        a = a.reshape(4 * own, -1)
        w = w.reshape(2, 16 * r, 2 * HEAD)
        o = o.reshape(2, 16 * wo.shape[0], -1)
        place = lax.div(s, 4) * (4 * own) + jnp.arange(4 * own)
        kv, q = matmul(a, w[0]), matmul(a, w[1])
        k = turned(kv[:, None, :HEAD], place, THETA)[:, 0]
        q = turned(q.reshape(4 * own, 2, HEAD), place, THETA).reshape(4 * own, -1)
        seen = attended(q, jnp.concatenate([k, kv[:, HEAD:]], -1), own)
        y = jnp.concatenate([jnp.dot(seen, o[i], preferred_element_type=jnp.float32) for i in (0, 1)], -1)
        return (x.astype(jnp.float32) + y).astype(jnp.bfloat16)

    tokens, whole = P(("dp", "sp"), None), P("sp", None)
    return jax.shard_map(
        step,
        mesh=mesh,
        in_specs=(tokens, P(None), whole, whole, whole, whole),
        out_specs=tokens,
        check_vma=False,
    )
```

```python
import functools

import jax
import jax.numpy as jnp
from jax import lax
from jax.experimental import pallas as pl
from jax.experimental.pallas import tpu as pltpu
from jax.sharding import PartitionSpec as P

NEG = -1e30
HIDDEN = 2 * NEG
LOG2E = 1.4426950408889634
VMEM = 63 * 2**20
HEAD = 256
THETA = 10000
MESH = pl.DeviceIdType.MESH


def _dot(a, b, ca, cb):
    return lax.dot_general(a, b, (((ca,), (cb,)), ((), ())), preferred_element_type=jnp.float32)


def flip(s, k):
    for bit in (1, 2, 4, 8):
        if k & bit:
            s = s + bit - 2 * bit * lax.rem(lax.div(s, bit), 2)
    return s


def meet(s, d, ks, across):
    barrier = pltpu.get_barrier_semaphore()
    for k in ks:
        pl.semaphore_signal(barrier, inc=1, device_id={"sp": flip(s, k)}, device_id_type=MESH)
    if across:
        pl.semaphore_signal(barrier, inc=1, device_id={"dp": 1 - d}, device_id_type=MESH)
    pl.semaphore_wait(barrier, len(ks) + across)


ROWS = 4
STRIP = 512
DMA = pltpu.SemaphoreType.DMA
SEMS = dict(
    xl=DMA((ROWS,)), wl=DMA((4,)), w1=DMA((2, 4, 3)), wz=DMA((2, 2)), wy=DMA((2, 2, 2)), wx=DMA((2, 2, 3)), a2=DMA((2, ROWS)), a1=DMA((2, ROWS)),
    af=DMA((2, ROWS)), kv=DMA((2, 3, 4)), o1=DMA((2,)), o2=DMA((2, 2)), o3=DMA((2, 4)), ox=DMA((2, 7)), od=DMA((2, 2, 8)), ol=DMA, back=DMA((2, 3)),
    bl=DMA,
)


def layer(x_ref, gain_ref, wq_ref, wk_ref, wv_ref, wo_ref, cos_ref, sin_ref, seen_ref, wide_ref,
          x_s, a_s, w_s, q_s, kv_s, got, top_s, mix_s, out_s, gap_s, *sems):
    sem = dict(zip(SEMS, sems))
    s, d = lax.axis_index("sp"), lax.axis_index("dp")
    other = 1 - d
    g, zh, y = lax.rem(s, 4), lax.rem(lax.div(s, 4), 2), lax.div(s, 8)
    own = x_ref.shape[0]
    r = wk_ref.shape[0]
    e = HEAD**-0.5 * LOG2E
    sends = []

    def send(src, dst, pair, at, to, when=None):
        copy = pltpu.make_async_remote_copy(src_ref=src, dst_ref=dst, send_sem=pair.at[(0, *at)], recv_sem=pair.at[(1, *at)], device_id=to,
                                            device_id_type=MESH)
        if when is None:
            copy.start()
        else:
            pl.when(when)(copy.start)
        sends.append((copy, when))

    def arrived(dst, pair, at):
        pltpu.make_async_copy(dst, dst, pair.at[(1, *at)]).wait()

    def keep(src, dst, at):
        copy = pltpu.make_async_copy(src, dst, at)
        copy.start()
        return copy

    sp = lambda k: {"sp": flip(s, k)}
    across = {"dp": other}
    meet(s, d, (1, 2, 3, 4, 8), True)

    def head(part, g):
        if part < 2:
            return (wk_ref, wv_ref)[part].at[:, pl.ds(pl.multiple_of(g * HEAD, HEAD), HEAD)]
        return wq_ref.at[:, pl.ds(pl.multiple_of(g * 2 * HEAD + (part - 2) * HEAD, HEAD), HEAD)]

    def rows_of(part, t, n=1):
        return w_s.at[part // 2, pl.ds(pl.multiple_of(t * r, 32), n * r), pl.ds(part % 2 * HEAD, HEAD)]

    def mine(group, k):
        return w_s.at[group, pl.ds(pl.multiple_of(lax.div(flip(s, 4 * k), 4) * (4 * r), 128), 4 * r), pl.ds(pl.multiple_of(d * HEAD, HEAD), HEAD)]

    def theirs(group, k):
        return w_s.at[group, pl.ds(pl.multiple_of(lax.div(flip(s, 4 * k), 4) * (4 * r), 128), 4 * r), pl.ds(pl.multiple_of(other * HEAD, HEAD), HEAD)]

    loads = [keep(x_ref.at[pl.ds(i * (own // ROWS), own // ROWS)], x_s.at[pl.ds(i * (own // ROWS), own // ROWS)], sem["xl"].at[i]) for i in range(ROWS)]
    for part in range(4):
        for m in (2, 3, 1):
            send(head(part, flip(g, m)), rows_of(part, s), sem["w1"], (part, m - 1), sp(m))
    kept = [keep(head(part, g), rows_of(part, s), sem["wl"].at[part]) for part in range(4)]
    kept_o = keep(wo_ref, wide_ref.at[pl.ds(pl.multiple_of(s * wo_ref.shape[0], 128), wo_ref.shape[0])], sem["ol"])

    n = own // ROWS
    gain = gain_ref[...].astype(jnp.float32)
    slot = lambda t, i=0, n=own: a_s.at[pl.ds(pl.multiple_of(t * own + i * n, n), n)]
    for i in range(ROWS):
        loads[i].wait()
        wide = x_s[i * n : (i + 1) * n, :].astype(jnp.float32)
        scale = lax.rsqrt(jnp.mean(wide * wide, -1, keepdims=True) + 1e-6)
        a_s[pl.ds(pl.multiple_of(g * own + i * n, n), n), :] = (wide * scale * gain).astype(jnp.bfloat16)
    gap_s[...] = lax.broadcasted_iota(jnp.int32, gap_s.shape, 1) - lax.broadcasted_iota(jnp.int32, gap_s.shape, 0)
    top_s[...] = jnp.full(top_s.shape, NEG, jnp.float32)
    mix_s[...] = jnp.zeros(mix_s.shape, jnp.float32)
    for i in range(ROWS):
        send(slot(g, i, n), slot(g, i, n), sem["a1"], (i,), sp(1))
    for copy in kept:
        copy.wait()
    for group in (0, 1):
        for part in (2 * group, 2 * group + 1):
            for m in (1, 2, 3):
                arrived(rows_of(part, flip(s, m)), sem["w1"], (part, m - 1))
        send(mine(group, 0), mine(group, 0), sem["wz"], (group,), sp(4))
        send(mine(group, 0), mine(group, 0), sem["wy"], (group, 0), sp(8))
    for i in range(ROWS):
        send(slot(g, i, n), slot(g, i, n), sem["a2"], (i,), sp(2))

    orows, ocols = wo_ref.shape[0], wo_ref.shape[1] // 2
    half = lambda t, h: wide_ref.at[pl.ds(pl.multiple_of(flip(s, t) * orows, 128), orows), pl.ds(pl.multiple_of(h * ocols, 128), ocols)]
    EVEN = (0, 4, 2, 6, 8, 12, 10, 14)
    kept_o.wait()
    send(half(0, d), half(0, d), sem["o1"], (), sp(4))
    send(half(0, d), half(0, d), sem["o2"], (0,), sp(2))

    def pass_on(group):
        arrived(mine(group, 2), sem["wy"], (group, 0))
        send(mine(group, 2), mine(group, 2), sem["wx"], (group, 0), across)
        arrived(mine(group, 1), sem["wz"], (group,))
        send(mine(group, 1), mine(group, 1), sem["wy"], (group, 1), sp(8))
        send(mine(group, 1), mine(group, 1), sem["wx"], (group, 1), across)
        arrived(mine(group, 3), sem["wy"], (group, 1))
        send(mine(group, 3), mine(group, 3), sem["wx"], (group, 2), across)

    def complete(group):
        for i, k in enumerate((2, 1, 3)):
            arrived(theirs(group, k), sem["wx"], (group, i))

    place = lambda c: lax.rem(lax.div(g, 2) * 2 + c, 4)
    rows = lambda c: pl.ds(pl.multiple_of(place(c) * own, own), own)

    def turn(t, at):
        half = HEAD // 2
        t = t.astype(jnp.bfloat16).astype(jnp.float32)
        a, b, cos, sin = t[:, :half], t[:, half:], cos_ref[at, :], sin_ref[at, :]
        return (a * cos - b * sin).astype(jnp.bfloat16), (b * cos + a * sin).astype(jnp.bfloat16)

    def project(group, c):
        at = rows(c)
        half = HEAD // 2
        t = _dot(a_s[at, :], w_s[group], 1, 0)
        into = (kv_s, q_s)[group]
        into[at, :half], into[at, half:HEAD] = turn(t[:, :HEAD], at)
        if group == 0:
            into[at, HEAD:] = t[:, HEAD:].astype(jnp.bfloat16)
        else:
            into[at, HEAD : HEAD + half], into[at, HEAD + half :] = turn(t[:, HEAD:], at)

    to_z = (y == 0) | (zh == 0)
    from_z = (y == 0) | (zh == 1)

    def exchange(kind, c, src, k):
        return pltpu.make_async_remote_copy(src_ref=src.at[rows(c)], dst_ref=got.at[kind, rows(c)], send_sem=sem["kv"].at[0, kind, c],
                                            recv_sem=sem["kv"].at[1, kind, c], device_id=sp(k), device_id_type=MESH)

    def share(c):
        @pl.when(to_z)
        def _():
            exchange(1, c, kv_s, 4).start()

        @pl.when(y == 0)
        def _():
            exchange(0, c, kv_s, 8).start()

    def forward(c):
        @pl.when(y == 0)
        def _():
            here = got.at[1, rows(c)]
            pltpu.make_async_copy(here, here, sem["kv"].at[1, 1, c]).wait()
            exchange(2, c, got.at[1], 8).start()

    def keys_values(c, _):
        project(0, c)
        share(c)

    def queries(c, _):
        project(1, c)

    def relay(i):
        arrived(slot(flip(g, 2), i, n), sem["a2"], (i,))
        send(slot(flip(g, 2), i, n), slot(flip(g, 2), i, n), sem["af"], (i,), sp(1))

    pass_on(0)
    for i in range(ROWS):
        arrived(slot(flip(g, 1), i, n), sem["a1"], (i,))
    complete(0)
    lax.fori_loop(0, 2, keys_values, None)
    pass_on(1)
    relay(0)
    relay(1)
    complete(1)
    lax.fori_loop(0, 2, queries, None)
    forward(0)
    relay(2)
    relay(3)
    for i in range(ROWS):
        arrived(slot(flip(g, 3), i, n), sem["af"], (i,))
    lax.fori_loop(2, 4, keys_values, None)
    forward(1)

    def o_on(i, to_y, to_x):
        k = EVEN[i]
        if to_y:
            send(half(k, d), half(k, d), sem["o3"], (i,), sp(8))
        if to_x:
            send(half(k, d), half(k, d), sem["ox"], (i - 1,), across)
        send(half(k, d), half(k, d), sem["od"], (0, i), sp(1))

    arrived(half(4, d), sem["o1"], ())
    send(half(4, d), half(4, d), sem["o2"], (1,), sp(2))
    o_on(0, True, False)
    o_on(1, True, True)
    lax.fori_loop(2, 4, queries, None)

    ones = jnp.ones((8, own), jnp.bfloat16)
    pieces = [(i, h) for i in range(4) for h in range(2)]

    def block(keys, values, first):
        scores = [_dot(keys, q_s[i * STRIP : (i + 1) * STRIP, h * HEAD : (h + 1) * HEAD], 1, 1) for i, h in pieces]
        weights, keeps = [], []
        for at, ((i, h), sc) in enumerate(zip(pieces, scores)):
            cols = slice(at * STRIP, (at + 1) * STRIP)
            if first is not None:
                sc = jnp.where(gap_s[...] >= first - i * STRIP, sc, HIDDEN)
            old = top_s[:, cols]
            top = jnp.maximum(old, sc.max(axis=0, keepdims=True))
            top_s[:, cols] = top
            weights.append(jnp.exp2((sc - top) * e).astype(jnp.bfloat16))
            keeps.append(jnp.exp2((old - top) * e))
        turned_values = jnp.concatenate([values.T, ones], axis=0)
        for at, (p, keep) in enumerate(zip(weights, keeps)):
            cols = slice(at * STRIP, (at + 1) * STRIP)
            mix_s[:, cols] = mix_s[:, cols] * keep + _dot(turned_values, p, 1, 0)

    def own_block(i, _):
        at = pl.ds(pl.multiple_of(i * own, own), own)
        block(kv_s[at, :HEAD], kv_s[at, HEAD:], i * own)

    lax.fori_loop(0, 4, own_block, None)
    for i in (2, 3):
        arrived(half(EVEN[i], d), sem["o2"], (i - 2,))
        o_on(i, True, True)

    def visit(t, _):
        late, kind, c = lax.div(t, 6), lax.rem(lax.div(t, 2), 3), lax.rem(t, 2)
        c = c + 2 * late
        comes = jnp.where(kind == 1, ((y == 0) & (late == 1)) | ((y == 1) & (zh == 1)), y == 1)
        wanted = jnp.where(kind == 1, zh == 1, y == 1)

        @pl.when(comes)
        def _():
            here = got.at[kind, rows(c)]
            pltpu.make_async_copy(here, here, sem["kv"].at[1, kind, c]).wait()

        @pl.when((kind == 1) & (y == 0) & (late == 1))
        def _():
            exchange(2, c, got.at[1], 8).start()

        @pl.when(wanted)
        def _():
            block(got[kind, rows(c), :HEAD], got[kind, rows(c), HEAD:], None)

    lax.fori_loop(0, 6, visit, None)
    for i in (4, 5, 6, 7):
        arrived(half(EVEN[i], d), sem["o3"], (i - 4,))
        o_on(i, False, True)
    lax.fori_loop(6, 12, visit, None)

    for at, (i, h) in enumerate(pieces):
        cols = slice(at * STRIP, (at + 1) * STRIP)
        out = mix_s[:HEAD, cols] * (1 / mix_s[HEAD : HEAD + 1, cols])
        out_s[i, :, h * HEAD : (h + 1) * HEAD] = out.T.astype(jnp.bfloat16)
    columns = lambda t: seen_ref.at[:, pl.ds(pl.multiple_of(t * 2 * HEAD, 2 * HEAD), 2 * HEAD)]
    for m in (2, 3, 1):
        send(out_s.at[flip(g, m)], columns(g), sem["back"], (m - 1,), sp(m))
    kept_b = keep(out_s.at[g], columns(g), sem["bl"])
    send(half(0, other), half(0, other), sem["od"], (1, 0), sp(1))
    for i in range(1, 8):
        arrived(half(EVEN[i], other), sem["ox"], (i - 1,))
        send(half(EVEN[i], other), half(EVEN[i], other), sem["od"], (1, i), sp(1))
    for i in range(8):
        arrived(half(EVEN[i] + 1, d), sem["od"], (0, i))
        arrived(half(EVEN[i] + 1, other), sem["od"], (1, i))
    for m in (1, 2, 3):
        arrived(columns(flip(g, m)), sem["back"], (m - 1,))
    kept_b.wait()
    for copy, _ in sends:
        copy.wait_send()

    for c in range(4):
        @pl.when(to_z)
        def _():
            exchange(1, c, kv_s, 4).wait_send()

        @pl.when(y == 0)
        def _():
            exchange(0, c, kv_s, 8).wait_send()
            exchange(2, c, got.at[1], 8).wait_send()


def attended(x, gain, wq, wk, wv, wo, cos, sin):
    own, width = x.shape
    bf16, f32 = jnp.bfloat16, jnp.float32
    vmem, hbm = pl.BlockSpec(memory_space=pltpu.VMEM), pl.BlockSpec(memory_space=pl.ANY)
    return pl.pallas_call(
        layer,
        out_shape=[jax.ShapeDtypeStruct((own, 4 * 2 * HEAD), bf16), jax.ShapeDtypeStruct((16 * wo.shape[0], wo.shape[1]), bf16)],
        in_specs=[hbm, vmem, hbm, hbm, hbm, vmem, vmem, vmem],
        out_specs=[hbm] * 2,
        scratch_shapes=[
            pltpu.VMEM((own, width), bf16),
            pltpu.VMEM((4 * own, width), bf16),
            pltpu.VMEM((2, 16 * wk.shape[0], 2 * HEAD), bf16),
            pltpu.VMEM((4 * own, 2 * HEAD), bf16),
            pltpu.VMEM((4 * own, 2 * HEAD), bf16),
            pltpu.VMEM((3, 4 * own, 2 * HEAD), bf16),
            pltpu.VMEM((1, 8 * own), f32),
            pltpu.VMEM((HEAD + 8, 8 * own), f32),
            pltpu.VMEM((4, own, 2 * HEAD), bf16),
            pltpu.VMEM((own, STRIP), jnp.int32),
            *SEMS.values(),
        ],
        compiler_params=pltpu.CompilerParams(collective_id=0, has_side_effects=True, vmem_limit_bytes=VMEM),
    )(x, gain, wq, wk, wv, wo, cos, sin)


def solution(mesh):
    def step(x, gain, wq, wk, wv, wo):
        tokens, half = 4 * x.shape[0], HEAD // 2
        place = lax.div(lax.axis_index("sp"), 4) * tokens + jnp.arange(tokens)
        angle = place.astype(jnp.float32)[:, None] * THETA ** (-jnp.arange(half, dtype=jnp.float32) / half)
        seen, wide = attended(x, gain[None], wq, wk, wv, wo, jnp.cos(angle), jnp.sin(angle))
        y = jnp.dot(seen, wide, preferred_element_type=jnp.float32)
        return (x.astype(jnp.float32) + y).astype(jnp.bfloat16)

    tokens, whole = P(("dp", "sp"), None), P("sp", None)
    return jax.shard_map(
        step,
        mesh=mesh,
        in_specs=(tokens, P(None), whole, whole, whole, whole),
        out_specs=tokens,
        check_vma=False,
    )
```

```python
import functools

import jax
import jax.numpy as jnp
from jax import lax
from jax.experimental import pallas as pl
from jax.experimental.pallas import tpu as pltpu
from jax.sharding import PartitionSpec as P

NEG = -1e30
HIDDEN = 2 * NEG
LOG2E = 1.4426950408889634
VMEM = 63 * 2**20
HEAD = 256
THETA = 10000
MESH = pl.DeviceIdType.MESH


def _dot(a, b, ca, cb):
    return lax.dot_general(a, b, (((ca,), (cb,)), ((), ())), preferred_element_type=jnp.float32)


def flip(s, k):
    for bit in (1, 2, 4, 8):
        if k & bit:
            s = s + bit - 2 * bit * lax.rem(lax.div(s, bit), 2)
    return s


def meet(s, d, ks, across):
    barrier = pltpu.get_barrier_semaphore()
    for k in ks:
        pl.semaphore_signal(barrier, inc=1, device_id={"sp": flip(s, k)}, device_id_type=MESH)
    if across:
        pl.semaphore_signal(barrier, inc=1, device_id={"dp": 1 - d}, device_id_type=MESH)
    pl.semaphore_wait(barrier, len(ks) + across)


ROWS = 4
STRIP = 512
DMA = pltpu.SemaphoreType.DMA
SEMS = dict(
    xl=DMA((ROWS,)), wl=DMA((4,)), w1=DMA((2, 4, 3)), wz=DMA((2, 2)), wy=DMA((2, 2, 2)), wx=DMA((2, 2, 4)), a2=DMA((2, ROWS)), a1=DMA((2, ROWS)),
    af=DMA((2, ROWS)), kv=DMA((2, 3, 4)), o1=DMA((2, 3)), o3=DMA((2, 4)), ox=DMA((2, 7)), od=DMA((2, 2, 8)), ol=DMA, back=DMA((2, 3)),
    bl=DMA,
)


def layer(x_ref, gain_ref, wq_ref, wk_ref, wv_ref, wo_ref, freq_ref, seen_ref, wide_ref,
          x_s, cos_s, sin_s, a_s, w_s, q_s, kv_s, got, top_s, mix_s, out_s, gap_s, *sems):
    sem = dict(zip(SEMS, sems))
    s, d = lax.axis_index("sp"), lax.axis_index("dp")
    other = 1 - d
    g, zh, y = lax.rem(s, 4), lax.rem(lax.div(s, 4), 2), lax.div(s, 8)
    own = x_ref.shape[0]
    r = wk_ref.shape[0]
    e = HEAD**-0.5 * LOG2E
    sends = []

    def send(src, dst, pair, at, to, when=None):
        copy = pltpu.make_async_remote_copy(src_ref=src, dst_ref=dst, send_sem=pair.at[(0, *at)], recv_sem=pair.at[(1, *at)], device_id=to,
                                            device_id_type=MESH)
        if when is None:
            copy.start()
        else:
            pl.when(when)(copy.start)
        sends.append((copy, when))

    def arrived(dst, pair, at):
        pltpu.make_async_copy(dst, dst, pair.at[(1, *at)]).wait()

    def keep(src, dst, at):
        copy = pltpu.make_async_copy(src, dst, at)
        copy.start()
        return copy

    sp = lambda k: {"sp": flip(s, k)}
    across = {"dp": other}
    meet(s, d, (1, 2, 3, 4, 8), True)

    def head(part, g):
        if part < 2:
            return (wk_ref, wv_ref)[part].at[:, pl.ds(pl.multiple_of(g * HEAD, HEAD), HEAD)]
        return wq_ref.at[:, pl.ds(pl.multiple_of(g * 2 * HEAD + (part - 2) * HEAD, HEAD), HEAD)]

    def rows_of(part, t, n=1):
        return w_s.at[part // 2, pl.ds(pl.multiple_of(t * r, 32), n * r), pl.ds(part % 2 * HEAD, HEAD)]

    def mine(group, k):
        return w_s.at[group, pl.ds(pl.multiple_of(lax.div(flip(s, 4 * k), 4) * (4 * r), 128), 4 * r), pl.ds(pl.multiple_of(d * HEAD, HEAD), HEAD)]

    def theirs(group, k):
        return w_s.at[group, pl.ds(pl.multiple_of(lax.div(flip(s, 4 * k), 4) * (4 * r), 128), 4 * r), pl.ds(pl.multiple_of(other * HEAD, HEAD), HEAD)]

    loads = [keep(x_ref.at[pl.ds(i * (own // ROWS), own // ROWS)], x_s.at[pl.ds(i * (own // ROWS), own // ROWS)], sem["xl"].at[i]) for i in range(ROWS)]
    def first_stage(part, m):
        return pltpu.make_async_remote_copy(src_ref=head(part, flip(g, m)), dst_ref=rows_of(part, s), send_sem=sem["w1"].at[0, part, m - 1],
                                            recv_sem=sem["w1"].at[1, part, m - 1], device_id=sp(m), device_id_type=MESH)

    for group in (0, 1):
        for m in (2, 3):
            for i in (0, 1):
                @pl.when(d == i)
                def _():
                    first_stage(2 * group + i, m).start()
        for part in (2 * group, 2 * group + 1):
            first_stage(part, 1).start()
    kept = [keep(head(part, g), rows_of(part, s), sem["wl"].at[part]) for part in range(4)]
    kept_o = keep(wo_ref, wide_ref.at[pl.ds(pl.multiple_of(s * wo_ref.shape[0], 128), wo_ref.shape[0])], sem["ol"])

    n = own // ROWS
    gain = gain_ref[...].astype(jnp.float32)
    slot = lambda t, i=0, n=own: a_s.at[pl.ds(pl.multiple_of(t * own + i * n, n), n)]
    for i in range(ROWS):
        loads[i].wait()
        wide = x_s[i * n : (i + 1) * n, :].astype(jnp.float32)
        scale = lax.rsqrt(jnp.mean(wide * wide, -1, keepdims=True) + 1e-6)
        a_s[pl.ds(pl.multiple_of(g * own + i * n, n), n), :] = (wide * scale * gain).astype(jnp.bfloat16)
    gap_s[...] = lax.broadcasted_iota(jnp.int32, gap_s.shape, 1) - lax.broadcasted_iota(jnp.int32, gap_s.shape, 0)
    top_s[...] = jnp.full(top_s.shape, NEG, jnp.float32)
    mix_s[...] = jnp.zeros(mix_s.shape, jnp.float32)
    for i in range(ROWS):
        send(slot(g, i, n), slot(g, i, n), sem["a1"], (i,), sp(1))
    for copy in kept:
        copy.wait()

    def near(group, h):
        return w_s.at[group, pl.ds(pl.multiple_of(lax.div(flip(s, 2), 2) * (2 * r), 64), 2 * r), pl.ds(pl.multiple_of(h * HEAD, HEAD), HEAD)]

    def from_cluster(group):
        for part in (2 * group, 2 * group + 1):
            arrived(rows_of(part, flip(s, 1)), sem["w1"], (part, 0))
        for i in (0, 1):
            @pl.when(d == i)
            def _():
                for m in (2, 3):
                    arrived(rows_of(2 * group + i, flip(s, m)), sem["w1"], (2 * group + i, m - 1))

    from_cluster(0)
    send(mine(0, 0), mine(0, 0), sem["wz"], (0,), sp(4))
    send(mine(0, 0), mine(0, 0), sem["wy"], (0, 0), sp(8))
    send(near(0, d), near(0, d), sem["wx"], (0, 3), across)
    for i in range(ROWS):
        send(slot(g, i, n), slot(g, i, n), sem["a2"], (i,), sp(2))
    from_cluster(1)
    send(mine(1, 0), mine(1, 0), sem["wz"], (1,), sp(4))
    send(mine(1, 0), mine(1, 0), sem["wy"], (1, 0), sp(8))
    send(near(1, d), near(1, d), sem["wx"], (1, 3), across)

    orows, ocols = wo_ref.shape[0], wo_ref.shape[1] // 2
    half = lambda t, h: wide_ref.at[pl.ds(pl.multiple_of(flip(s, t) * orows, 128), orows), pl.ds(pl.multiple_of(h * ocols, 128), ocols)]
    EVEN = (0, 2, 4, 6, 8, 10, 12, 14)
    kept_o.wait()
    for i in (1, 2, 3):
        send(half(0, d), half(0, d), sem["o1"], (i - 1,), sp(EVEN[i]))

    def o_on(i, to_y=False):
        k = EVEN[i]
        if to_y:
            send(half(k, d), half(k, d), sem["o3"], (i,), sp(8))
        if i:
            send(half(k, d), half(k, d), sem["ox"], (i - 1,), across)
        send(half(k, d), half(k, d), sem["od"], (0, i), sp(1))

    o_on(0, True)

    for i in range(4):
        spot = (lax.div(s, 4) * 4 + i) * own + lax.broadcasted_iota(jnp.int32, (own, HEAD // 2), 0)
        angle = spot.astype(jnp.float32) * freq_ref[...]
        cos_s[i * own : (i + 1) * own, :] = jnp.cos(angle)
        sin_s[i * own : (i + 1) * own, :] = jnp.sin(angle)

    def pass_y(group):
        arrived(mine(group, 2), sem["wy"], (group, 0))
        send(mine(group, 2), mine(group, 2), sem["wx"], (group, 0), across)

    def pass_z(group):
        arrived(mine(group, 1), sem["wz"], (group,))
        send(mine(group, 1), mine(group, 1), sem["wy"], (group, 1), sp(8))
        send(mine(group, 1), mine(group, 1), sem["wx"], (group, 1), across)
        arrived(mine(group, 3), sem["wy"], (group, 1))
        send(mine(group, 3), mine(group, 3), sem["wx"], (group, 2), across)

    def complete(group):
        for i, k in enumerate((2, 1, 3)):
            arrived(theirs(group, k), sem["wx"], (group, i))
        arrived(near(group, other), sem["wx"], (group, 3))

    place = lambda c: lax.rem(lax.div(g, 2) * 2 + c, 4)
    rows = lambda c: pl.ds(pl.multiple_of(place(c) * own, own), own)

    def turn(t, at):
        half = HEAD // 2
        t = t.astype(jnp.bfloat16).astype(jnp.float32)
        a, b, cos, sin = t[:, :half], t[:, half:], cos_s[at, :], sin_s[at, :]
        return (a * cos - b * sin).astype(jnp.bfloat16), (b * cos + a * sin).astype(jnp.bfloat16)

    def project(group, c):
        at = rows(c)
        half = HEAD // 2
        t = _dot(a_s[at, :], w_s[group], 1, 0)
        into = (kv_s, q_s)[group]
        into[at, :half], into[at, half:HEAD] = turn(t[:, :HEAD], at)
        if group == 0:
            into[at, HEAD:] = t[:, HEAD:].astype(jnp.bfloat16)
        else:
            into[at, HEAD : HEAD + half], into[at, HEAD + half :] = turn(t[:, HEAD:], at)

    to_z = (y == 0) | (zh == 0)
    from_z = (y == 0) | (zh == 1)

    def exchange(kind, c, src, k):
        return pltpu.make_async_remote_copy(src_ref=src.at[rows(c)], dst_ref=got.at[kind, rows(c)], send_sem=sem["kv"].at[0, kind, c],
                                            recv_sem=sem["kv"].at[1, kind, c], device_id=sp(k), device_id_type=MESH)

    def share_z(c):
        @pl.when(to_z)
        def _():
            exchange(1, c, kv_s, 4).start()

    def share_y(c):
        @pl.when(y == 0)
        def _():
            exchange(0, c, kv_s, 8).start()

    def forward(c):
        @pl.when(y == 0)
        def _():
            here = got.at[1, rows(c)]
            pltpu.make_async_copy(here, here, sem["kv"].at[1, 1, c]).wait()
            exchange(2, c, got.at[1], 8).start()

    def early(c, _):
        project(0, c)
        share_y(c)

    def late(c, _):
        project(0, c)
        share_z(c)
        share_y(c)

    def queries(c, _):
        project(1, c)

    def relay(i):
        arrived(slot(flip(g, 2), i, n), sem["a2"], (i,))
        send(slot(flip(g, 2), i, n), slot(flip(g, 2), i, n), sem["af"], (i,), sp(1))

    pass_y(0)
    pass_z(0)
    for i in range(ROWS):
        arrived(slot(flip(g, 1), i, n), sem["a1"], (i,))
    complete(0)
    lax.fori_loop(0, 2, early, None)
    pass_y(1)
    arrived(half(8, d), sem["o3"], (0,))
    o_on(4)
    for i in range(ROWS):
        relay(i)
    share_z(0)
    share_z(1)
    for i in range(ROWS):
        arrived(slot(flip(g, 3), i, n), sem["af"], (i,))
    lax.fori_loop(2, 4, late, None)
    pass_z(1)
    for i in (1, 2, 3):
        arrived(half(EVEN[i], d), sem["o1"], (i - 1,))
        o_on(i, True)
    complete(1)
    lax.fori_loop(0, 4, queries, None)
    forward(0)
    forward(1)

    ones = jnp.ones((8, own), jnp.bfloat16)
    def block(keys, values, first=None):
        pieces = [(i, h) for i in range(first or 0, 4) for h in range(2)]
        scores = [_dot(keys, q_s[i * STRIP : (i + 1) * STRIP, h * HEAD : (h + 1) * HEAD], 1, 1) for i, h in pieces]
        weights, keeps = [], []
        for (i, h), sc in zip(pieces, scores):
            cols = slice((2 * i + h) * STRIP, (2 * i + h + 1) * STRIP)
            if i == first:
                sc = jnp.where(gap_s[...] >= 0, sc, HIDDEN)
            old = top_s[:, cols]
            top = jnp.maximum(old, sc.max(axis=0, keepdims=True))
            top_s[:, cols] = top
            weights.append(jnp.exp2((sc - top) * e).astype(jnp.bfloat16))
            keeps.append(jnp.exp2((old - top) * e))
        turned_values = jnp.concatenate([values.T, ones], axis=0)
        for (i, h), p, keep in zip(pieces, weights, keeps):
            cols = slice((2 * i + h) * STRIP, (2 * i + h + 1) * STRIP)
            mix_s[:, cols] = mix_s[:, cols] * keep + _dot(turned_values, p, 1, 0)

    for i in range(4):
        block(kv_s[i * own : (i + 1) * own, :HEAD], kv_s[i * own : (i + 1) * own, HEAD:], i)
    for i in (5, 6, 7):
        arrived(half(EVEN[i], d), sem["o3"], (i - 4,))
        o_on(i)

    def visit(t, _):
        late, kind, c = lax.div(t, 6), lax.rem(lax.div(t, 2), 3), lax.rem(t, 2)
        c = c + 2 * late
        comes = jnp.where(kind == 1, ((y == 0) & (late == 1)) | ((y == 1) & (zh == 1)), y == 1)
        wanted = jnp.where(kind == 1, zh == 1, y == 1)

        @pl.when(comes)
        def _():
            here = got.at[kind, rows(c)]
            pltpu.make_async_copy(here, here, sem["kv"].at[1, kind, c]).wait()

        @pl.when((kind == 1) & (y == 0) & (late == 1))
        def _():
            exchange(2, c, got.at[1], 8).start()

        @pl.when(wanted)
        def _():
            block(got[kind, rows(c), :HEAD], got[kind, rows(c), HEAD:])

    lax.fori_loop(0, 12, visit, None)

    for at in range(8):
        i, h, cols = at // 2, at % 2, slice(at * STRIP, (at + 1) * STRIP)
        out = mix_s[:HEAD, cols] * (1 / mix_s[HEAD : HEAD + 1, cols])
        out_s[i, :, h * HEAD : (h + 1) * HEAD] = out.T.astype(jnp.bfloat16)
    columns = lambda t: seen_ref.at[:, pl.ds(pl.multiple_of(t * 2 * HEAD, 2 * HEAD), 2 * HEAD)]
    for m in (2, 3, 1):
        send(out_s.at[flip(g, m)], columns(g), sem["back"], (m - 1,), sp(m))
    kept_b = keep(out_s.at[g], columns(g), sem["bl"])
    send(half(0, other), half(0, other), sem["od"], (1, 0), sp(1))
    for i in range(1, 8):
        arrived(half(EVEN[i], other), sem["ox"], (i - 1,))
        send(half(EVEN[i], other), half(EVEN[i], other), sem["od"], (1, i), sp(1))
    for i in range(8):
        arrived(half(EVEN[i] + 1, d), sem["od"], (0, i))
        arrived(half(EVEN[i] + 1, other), sem["od"], (1, i))
    for m in (1, 2, 3):
        arrived(columns(flip(g, m)), sem["back"], (m - 1,))
    kept_b.wait()
    for copy, _ in sends:
        copy.wait_send()
    for group in (0, 1):
        for i in (0, 1):
            @pl.when(d == i)
            def _():
                for m in (2, 3):
                    first_stage(2 * group + i, m).wait_send()
        for part in (2 * group, 2 * group + 1):
            first_stage(part, 1).wait_send()

    for c in range(4):
        @pl.when(to_z)
        def _():
            exchange(1, c, kv_s, 4).wait_send()

        @pl.when(y == 0)
        def _():
            exchange(0, c, kv_s, 8).wait_send()
            exchange(2, c, got.at[1], 8).wait_send()


def attended(x, gain, wq, wk, wv, wo, freq):
    own, width = x.shape
    bf16, f32 = jnp.bfloat16, jnp.float32
    vmem, hbm = pl.BlockSpec(memory_space=pltpu.VMEM), pl.BlockSpec(memory_space=pl.ANY)
    return pl.pallas_call(
        layer,
        out_shape=[jax.ShapeDtypeStruct((own, 4 * 2 * HEAD), bf16), jax.ShapeDtypeStruct((16 * wo.shape[0], wo.shape[1]), bf16)],
        in_specs=[hbm, vmem, hbm, hbm, hbm, vmem, vmem],
        out_specs=[hbm] * 2,
        scratch_shapes=[
            pltpu.VMEM((own, width), bf16),
            pltpu.VMEM((4 * own, HEAD // 2), f32),
            pltpu.VMEM((4 * own, HEAD // 2), f32),
            pltpu.VMEM((4 * own, width), bf16),
            pltpu.VMEM((2, 16 * wk.shape[0], 2 * HEAD), bf16),
            pltpu.VMEM((4 * own, 2 * HEAD), bf16),
            pltpu.VMEM((4 * own, 2 * HEAD), bf16),
            pltpu.VMEM((3, 4 * own, 2 * HEAD), bf16),
            pltpu.VMEM((1, 8 * own), f32),
            pltpu.VMEM((HEAD + 8, 8 * own), f32),
            pltpu.VMEM((4, own, 2 * HEAD), bf16),
            pltpu.VMEM((own, STRIP), jnp.int32),
            *SEMS.values(),
        ],
        compiler_params=pltpu.CompilerParams(collective_id=0, has_side_effects=True, vmem_limit_bytes=VMEM),
    )(x, gain, wq, wk, wv, wo, freq)


def solution(mesh):
    def step(x, gain, wq, wk, wv, wo):
        half = HEAD // 2
        freq = THETA ** (-jnp.arange(half, dtype=jnp.float32) / half)
        seen, wide = attended(x, gain, wq, wk, wv, wo, freq[None])
        y = jnp.dot(seen, wide, preferred_element_type=jnp.float32)
        return (x.astype(jnp.float32) + y).astype(jnp.bfloat16)

    tokens, whole = P(("dp", "sp"), None), P("sp", None)
    return jax.shard_map(
        step,
        mesh=mesh,
        in_specs=(tokens, P(None), whole, whole, whole, whole),
        out_specs=tokens,
        check_vma=False,
    )
```

```python
import functools

import jax
import jax.numpy as jnp
from jax import lax
from jax.experimental import pallas as pl
from jax.experimental.pallas import tpu as pltpu
from jax.sharding import PartitionSpec as P

NEG = -1e30
HIDDEN = 2 * NEG
LOG2E = 1.4426950408889634
VMEM = 63 * 2**20
HEAD = 256
THETA = 10000
MESH = pl.DeviceIdType.MESH


def _dot(a, b, ca, cb):
    return lax.dot_general(a, b, (((ca,), (cb,)), ((), ())), preferred_element_type=jnp.float32)


def flip(s, k):
    for bit in (1, 2, 4, 8):
        if k & bit:
            s = s + bit - 2 * bit * lax.rem(lax.div(s, bit), 2)
    return s


def meet(s, d, ks, across):
    barrier = pltpu.get_barrier_semaphore()
    for k in ks:
        pl.semaphore_signal(barrier, inc=1, device_id={"sp": flip(s, k)}, device_id_type=MESH)
    if across:
        pl.semaphore_signal(barrier, inc=1, device_id={"dp": 1 - d}, device_id_type=MESH)
    pl.semaphore_wait(barrier, len(ks) + across)


ROWS = 4
STRIP = 512
DMA = pltpu.SemaphoreType.DMA
SEMS = dict(
    xl=DMA((ROWS,)), wl=DMA((4,)), w1=DMA((2, 4, 3)), wz=DMA((2, 2)), wy=DMA((2, 2, 2)), wx=DMA((2, 2, 4)), a2=DMA((2, ROWS)), a1=DMA((2, ROWS)),
    af=DMA((2, ROWS)), kv=DMA((2, 3, 4)), o1=DMA((2, 5)), o3=DMA((2, 4)), ox=DMA((2, 7)), od=DMA((2, 2, 8)), ol=DMA, back=DMA((2, 3)),
    bl=DMA,
)


def layer(x_ref, gain_ref, wq_ref, wk_ref, wv_ref, wo_ref, freq_ref, seen_ref, wide_ref,
          x_s, cos_s, sin_s, a_s, w_s, q_s, kv_s, got, top_s, mix_s, out_s, gap_s, *sems):
    sem = dict(zip(SEMS, sems))
    s, d = lax.axis_index("sp"), lax.axis_index("dp")
    other = 1 - d
    g, zh, y = lax.rem(s, 4), lax.rem(lax.div(s, 4), 2), lax.div(s, 8)
    own = x_ref.shape[0]
    r = wk_ref.shape[0]
    e = HEAD**-0.5 * LOG2E
    sends = []

    def send(src, dst, pair, at, to, when=None):
        copy = pltpu.make_async_remote_copy(src_ref=src, dst_ref=dst, send_sem=pair.at[(0, *at)], recv_sem=pair.at[(1, *at)], device_id=to,
                                            device_id_type=MESH)
        if when is None:
            copy.start()
        else:
            pl.when(when)(copy.start)
        sends.append((copy, when))

    def arrived(dst, pair, at):
        pltpu.make_async_copy(dst, dst, pair.at[(1, *at)]).wait()

    def keep(src, dst, at):
        copy = pltpu.make_async_copy(src, dst, at)
        copy.start()
        return copy

    sp = lambda k: {"sp": flip(s, k)}
    across = {"dp": other}
    meet(s, d, (1, 2, 3, 4, 8), True)

    def head(part, g):
        if part < 2:
            return (wk_ref, wv_ref)[part].at[:, pl.ds(pl.multiple_of(g * HEAD, HEAD), HEAD)]
        return wq_ref.at[:, pl.ds(pl.multiple_of(g * 2 * HEAD + (part - 2) * HEAD, HEAD), HEAD)]

    def rows_of(part, t, n=1):
        return w_s.at[part // 2, pl.ds(pl.multiple_of(t * r, 32), n * r), pl.ds(part % 2 * HEAD, HEAD)]

    def mine(group, k):
        return w_s.at[group, pl.ds(pl.multiple_of(lax.div(flip(s, 4 * k), 4) * (4 * r), 128), 4 * r), pl.ds(pl.multiple_of(d * HEAD, HEAD), HEAD)]

    def theirs(group, k):
        return w_s.at[group, pl.ds(pl.multiple_of(lax.div(flip(s, 4 * k), 4) * (4 * r), 128), 4 * r), pl.ds(pl.multiple_of(other * HEAD, HEAD), HEAD)]

    loads = [keep(x_ref.at[pl.ds(i * (own // ROWS), own // ROWS)], x_s.at[pl.ds(i * (own // ROWS), own // ROWS)], sem["xl"].at[i]) for i in range(ROWS)]
    def first_stage(part, m):
        return pltpu.make_async_remote_copy(src_ref=head(part, flip(g, m)), dst_ref=rows_of(part, s), send_sem=sem["w1"].at[0, part, m - 1],
                                            recv_sem=sem["w1"].at[1, part, m - 1], device_id=sp(m), device_id_type=MESH)

    for group in (0, 1):
        for m in (2, 3):
            for i in (0, 1):
                @pl.when(d == i)
                def _():
                    first_stage(2 * group + i, m).start()
        for part in (2 * group, 2 * group + 1):
            first_stage(part, 1).start()
    kept = [keep(head(part, g), rows_of(part, s), sem["wl"].at[part]) for part in range(4)]
    kept_o = keep(wo_ref, wide_ref.at[pl.ds(pl.multiple_of(s * wo_ref.shape[0], 128), wo_ref.shape[0])], sem["ol"])

    n = own // ROWS
    gain = gain_ref[...].astype(jnp.float32)
    slot = lambda t, i=0, n=own: a_s.at[pl.ds(pl.multiple_of(t * own + i * n, n), n)]
    for i in range(ROWS):
        loads[i].wait()
        wide = x_s[i * n : (i + 1) * n, :].astype(jnp.float32)
        scale = lax.rsqrt(jnp.mean(wide * wide, -1, keepdims=True) + 1e-6)
        a_s[pl.ds(pl.multiple_of(g * own + i * n, n), n), :] = (wide * scale * gain).astype(jnp.bfloat16)
    gap_s[...] = lax.broadcasted_iota(jnp.int32, gap_s.shape, 1) - lax.broadcasted_iota(jnp.int32, gap_s.shape, 0)
    top_s[...] = jnp.full(top_s.shape, NEG, jnp.float32)
    mix_s[...] = jnp.zeros(mix_s.shape, jnp.float32)
    for i in range(ROWS):
        send(slot(g, i, n), slot(g, i, n), sem["a1"], (i,), sp(1))
    for copy in kept:
        copy.wait()

    def near(group, h):
        return w_s.at[group, pl.ds(pl.multiple_of(lax.div(flip(s, 2), 2) * (2 * r), 64), 2 * r), pl.ds(pl.multiple_of(h * HEAD, HEAD), HEAD)]

    def from_cluster(group):
        for part in (2 * group, 2 * group + 1):
            arrived(rows_of(part, flip(s, 1)), sem["w1"], (part, 0))
        for i in (0, 1):
            @pl.when(d == i)
            def _():
                for m in (2, 3):
                    arrived(rows_of(2 * group + i, flip(s, m)), sem["w1"], (2 * group + i, m - 1))

    def to_neighbour(i):
        send(slot(g, i, n), slot(g, i, n), sem["a2"], (i,), sp(2))

    for group in (0, 1):
        from_cluster(group)
        send(mine(group, 0), mine(group, 0), sem["wz"], (group,), sp(4))
        send(mine(group, 0), mine(group, 0), sem["wy"], (group, 0), sp(8))
        send(near(group, d), near(group, d), sem["wx"], (group, 3), across)
        if group == 0:
            to_neighbour(0)
            to_neighbour(1)

    orows, ocols = wo_ref.shape[0], wo_ref.shape[1] // 2
    half = lambda t, h: wide_ref.at[pl.ds(pl.multiple_of(flip(s, t) * orows, 128), orows), pl.ds(pl.multiple_of(h * ocols, 128), ocols)]
    EVEN = (0, 2, 4, 6, 8, 10, 12, 14)
    kept_o.wait()
    inner = lax.rem(lax.div(s, 2), 2) + zh == 1
    send(half(0, d), half(0, d), sem["o1"], (0,), sp(2))
    send(half(0, d), half(0, d), sem["o1"], (1,), sp(6), inner)
    to_neighbour(2)
    to_neighbour(3)

    def o_on(i, to_y=False):
        k = EVEN[i]
        if to_y:
            send(half(k, d), half(k, d), sem["o3"], (i,), sp(8))
        if i:
            send(half(k, d), half(k, d), sem["ox"], (i - 1,), across)
        send(half(k, d), half(k, d), sem["od"], (0, i), sp(1))

    o_on(0, True)

    for i in range(4):
        spot = (lax.div(s, 4) * 4 + i) * own + lax.broadcasted_iota(jnp.int32, (own, HEAD // 2), 0)
        angle = spot.astype(jnp.float32) * freq_ref[...]
        cos_s[i * own : (i + 1) * own, :] = jnp.cos(angle)
        sin_s[i * own : (i + 1) * own, :] = jnp.sin(angle)

    def pass_y(group):
        arrived(mine(group, 2), sem["wy"], (group, 0))
        send(mine(group, 2), mine(group, 2), sem["wx"], (group, 0), across)

    def pass_z(group):
        arrived(mine(group, 1), sem["wz"], (group,))
        send(mine(group, 1), mine(group, 1), sem["wy"], (group, 1), sp(8))
        send(mine(group, 1), mine(group, 1), sem["wx"], (group, 1), across)
        arrived(mine(group, 3), sem["wy"], (group, 1))
        send(mine(group, 3), mine(group, 3), sem["wx"], (group, 2), across)

    def complete(group):
        for i, k in enumerate((2, 1, 3)):
            arrived(theirs(group, k), sem["wx"], (group, i))
        arrived(near(group, other), sem["wx"], (group, 3))

    place = lambda c: lax.rem(lax.div(g, 2) * 2 + c, 4)
    rows = lambda c: pl.ds(pl.multiple_of(place(c) * own, own), own)

    def turn(t, at):
        half = HEAD // 2
        t = t.astype(jnp.bfloat16).astype(jnp.float32)
        a, b, cos, sin = t[:, :half], t[:, half:], cos_s[at, :], sin_s[at, :]
        return (a * cos - b * sin).astype(jnp.bfloat16), (b * cos + a * sin).astype(jnp.bfloat16)

    def project(group, c):
        at = rows(c)
        half = HEAD // 2
        t = _dot(a_s[at, :], w_s[group], 1, 0)
        into = (kv_s, q_s)[group]
        into[at, :half], into[at, half:HEAD] = turn(t[:, :HEAD], at)
        if group == 0:
            into[at, HEAD:] = t[:, HEAD:].astype(jnp.bfloat16)
        else:
            into[at, HEAD : HEAD + half], into[at, HEAD + half :] = turn(t[:, HEAD:], at)

    to_z = (y == 0) | (zh == 0)
    from_z = (y == 0) | (zh == 1)

    def exchange(kind, c, src, k):
        return pltpu.make_async_remote_copy(src_ref=src.at[rows(c)], dst_ref=got.at[kind, rows(c)], send_sem=sem["kv"].at[0, kind, c],
                                            recv_sem=sem["kv"].at[1, kind, c], device_id=sp(k), device_id_type=MESH)

    def share_z(c):
        @pl.when(to_z)
        def _():
            exchange(1, c, kv_s, 4).start()

    def share_y(c):
        @pl.when(y == 0)
        def _():
            exchange(0, c, kv_s, 8).start()

    def forward(c):
        @pl.when(y == 0)
        def _():
            here = got.at[1, rows(c)]
            pltpu.make_async_copy(here, here, sem["kv"].at[1, 1, c]).wait()
            exchange(2, c, got.at[1], 8).start()

    def early(c, _):
        project(0, c)
        share_y(c)
        pl.when(inner)(lambda: share_z(c))

    def late(c, _):
        project(0, c)
        share_z(c)
        share_y(c)

    def queries(c, _):
        project(1, c)

    def relay(i):
        arrived(slot(flip(g, 2), i, n), sem["a2"], (i,))
        send(slot(flip(g, 2), i, n), slot(flip(g, 2), i, n), sem["af"], (i,), sp(1))

    pass_y(0)
    pass_z(0)
    arrived(half(2, d), sem["o1"], (0,))
    send(half(2, d), half(2, d), sem["o1"], (2,), sp(6), inner)
    o_on(1, True)
    for i in range(ROWS):
        arrived(slot(flip(g, 1), i, n), sem["a1"], (i,))
    complete(0)
    lax.fori_loop(0, 2, early, None)
    pass_y(1)
    pass_z(1)
    arrived(half(8, d), sem["o3"], (0,))
    o_on(4)
    for i in range(ROWS):
        relay(i)

    @pl.when(jnp.logical_not(inner))
    def _():
        share_z(0)
        share_z(1)

    for i in range(ROWS):
        arrived(slot(flip(g, 3), i, n), sem["af"], (i,))
    lax.fori_loop(2, 4, late, None)
    for i, k in enumerate((6, 4)):
        pl.when(inner)(functools.partial(arrived, half(k, d), sem["o1"], (1 + i,)))
        send(half(k, d), half(k, d), sem["o1"], (3 + i,), sp(2), inner)
        pl.when(jnp.logical_not(inner))(functools.partial(arrived, half(10 - k, d), sem["o1"], (3 + i,)))
    o_on(2, True)
    o_on(3, True)
    complete(1)
    lax.fori_loop(0, 4, queries, None)
    forward(0)
    forward(1)

    ones = jnp.ones((8, own), jnp.bfloat16)
    def block(keys, values, first=None):
        pieces = [(i, h) for i in range(first or 0, 4) for h in range(2)]
        scores = [_dot(keys, q_s[i * STRIP : (i + 1) * STRIP, h * HEAD : (h + 1) * HEAD], 1, 1) for i, h in pieces]
        weights, keeps = [], []
        for (i, h), sc in zip(pieces, scores):
            cols = slice((2 * i + h) * STRIP, (2 * i + h + 1) * STRIP)
            if i == first:
                sc = jnp.where(gap_s[...] >= 0, sc, HIDDEN)
            old = top_s[:, cols]
            top = jnp.maximum(old, sc.max(axis=0, keepdims=True))
            top_s[:, cols] = top
            weights.append(jnp.exp2((sc - top) * e).astype(jnp.bfloat16))
            keeps.append(jnp.exp2((old - top) * e))
        turned_values = jnp.concatenate([values.T, ones], axis=0)
        for (i, h), p, keep in zip(pieces, weights, keeps):
            cols = slice((2 * i + h) * STRIP, (2 * i + h + 1) * STRIP)
            mix_s[:, cols] = mix_s[:, cols] * keep + _dot(turned_values, p, 1, 0)

    for i in range(4):
        block(kv_s[i * own : (i + 1) * own, :HEAD], kv_s[i * own : (i + 1) * own, HEAD:], i)

    def visit(t, _):
        late, kind, c = lax.div(t, 6), lax.rem(lax.div(t, 2), 3), lax.rem(t, 2)
        c = c + 2 * late
        comes = jnp.where(kind == 1, ((y == 0) & (late == 1)) | ((y == 1) & (zh == 1)), y == 1)
        wanted = jnp.where(kind == 1, zh == 1, y == 1)

        @pl.when(comes)
        def _():
            here = got.at[kind, rows(c)]
            pltpu.make_async_copy(here, here, sem["kv"].at[1, kind, c]).wait()

        @pl.when((kind == 1) & (y == 0) & (late == 1))
        def _():
            exchange(2, c, got.at[1], 8).start()

        @pl.when(wanted)
        def _():
            block(got[kind, rows(c), :HEAD], got[kind, rows(c), HEAD:])

    lax.fori_loop(0, 6, visit, None)
    for i in (5, 6, 7):
        arrived(half(EVEN[i], d), sem["o3"], (i - 4,))
        o_on(i)
    lax.fori_loop(6, 12, visit, None)

    for at in range(8):
        i, h, cols = at // 2, at % 2, slice(at * STRIP, (at + 1) * STRIP)
        out = mix_s[:HEAD, cols] * (1 / mix_s[HEAD : HEAD + 1, cols])
        out_s[i, :, h * HEAD : (h + 1) * HEAD] = out.T.astype(jnp.bfloat16)
    columns = lambda t: seen_ref.at[:, pl.ds(pl.multiple_of(t * 2 * HEAD, 2 * HEAD), 2 * HEAD)]
    for m in (2, 3, 1):
        send(out_s.at[flip(g, m)], columns(g), sem["back"], (m - 1,), sp(m))
    kept_b = keep(out_s.at[g], columns(g), sem["bl"])
    send(half(0, other), half(0, other), sem["od"], (1, 0), sp(1))
    for i in range(1, 8):
        arrived(half(EVEN[i], other), sem["ox"], (i - 1,))
        send(half(EVEN[i], other), half(EVEN[i], other), sem["od"], (1, i), sp(1))
    for i in range(8):
        arrived(half(EVEN[i] + 1, d), sem["od"], (0, i))
        arrived(half(EVEN[i] + 1, other), sem["od"], (1, i))
    for m in (1, 2, 3):
        arrived(columns(flip(g, m)), sem["back"], (m - 1,))
    kept_b.wait()
    for copy, when in sends:
        if when is None:
            copy.wait_send()
        else:
            pl.when(when)(copy.wait_send)
    for group in (0, 1):
        for i in (0, 1):
            @pl.when(d == i)
            def _():
                for m in (2, 3):
                    first_stage(2 * group + i, m).wait_send()
        for part in (2 * group, 2 * group + 1):
            first_stage(part, 1).wait_send()

    for c in range(4):
        @pl.when(to_z)
        def _():
            exchange(1, c, kv_s, 4).wait_send()

        @pl.when(y == 0)
        def _():
            exchange(0, c, kv_s, 8).wait_send()
            exchange(2, c, got.at[1], 8).wait_send()


def attended(x, gain, wq, wk, wv, wo, freq):
    own, width = x.shape
    bf16, f32 = jnp.bfloat16, jnp.float32
    vmem, hbm = pl.BlockSpec(memory_space=pltpu.VMEM), pl.BlockSpec(memory_space=pl.ANY)
    return pl.pallas_call(
        layer,
        out_shape=[jax.ShapeDtypeStruct((own, 4 * 2 * HEAD), bf16), jax.ShapeDtypeStruct((16 * wo.shape[0], wo.shape[1]), bf16)],
        in_specs=[hbm, vmem, hbm, hbm, hbm, vmem, vmem],
        out_specs=[hbm] * 2,
        scratch_shapes=[
            pltpu.VMEM((own, width), bf16),
            pltpu.VMEM((4 * own, HEAD // 2), f32),
            pltpu.VMEM((4 * own, HEAD // 2), f32),
            pltpu.VMEM((4 * own, width), bf16),
            pltpu.VMEM((2, 16 * wk.shape[0], 2 * HEAD), bf16),
            pltpu.VMEM((4 * own, 2 * HEAD), bf16),
            pltpu.VMEM((4 * own, 2 * HEAD), bf16),
            pltpu.VMEM((3, 4 * own, 2 * HEAD), bf16),
            pltpu.VMEM((1, 8 * own), f32),
            pltpu.VMEM((HEAD + 8, 8 * own), f32),
            pltpu.VMEM((4, own, 2 * HEAD), bf16),
            pltpu.VMEM((own, STRIP), jnp.int32),
            *SEMS.values(),
        ],
        compiler_params=pltpu.CompilerParams(collective_id=0, has_side_effects=True, vmem_limit_bytes=VMEM),
    )(x, gain, wq, wk, wv, wo, freq)


def solution(mesh):
    def step(x, gain, wq, wk, wv, wo):
        half = HEAD // 2
        freq = THETA ** (-jnp.arange(half, dtype=jnp.float32) / half)
        seen, wide = attended(x, gain, wq, wk, wv, wo, freq[None])
        y = jnp.dot(seen, wide, preferred_element_type=jnp.float32)
        return (x.astype(jnp.float32) + y).astype(jnp.bfloat16)

    tokens, whole = P(("dp", "sp"), None), P("sp", None)
    return jax.shard_map(
        step,
        mesh=mesh,
        in_specs=(tokens, P(None), whole, whole, whole, whole),
        out_specs=tokens,
        check_vma=False,
    )
```

```python
import functools

import jax
import jax.numpy as jnp
from jax import lax
from jax.experimental import pallas as pl
from jax.experimental.pallas import tpu as pltpu
from jax.sharding import PartitionSpec as P

NEG = -1e30
HIDDEN = 2 * NEG
LOG2E = 1.4426950408889634
VMEM = 63 * 2**20
HEAD = 256
THETA = 10000
MESH = pl.DeviceIdType.MESH


def _dot(a, b, ca, cb):
    return lax.dot_general(a, b, (((ca,), (cb,)), ((), ())), preferred_element_type=jnp.float32)


def flip(s, k):
    for bit in (1, 2, 4, 8):
        if k & bit:
            s = s + bit - 2 * bit * lax.rem(lax.div(s, bit), 2)
    return s


def meet(s, d, ks, across):
    barrier = pltpu.get_barrier_semaphore()
    for k in ks:
        pl.semaphore_signal(barrier, inc=1, device_id={"sp": flip(s, k)}, device_id_type=MESH)
    if across:
        pl.semaphore_signal(barrier, inc=1, device_id={"dp": 1 - d}, device_id_type=MESH)
    pl.semaphore_wait(barrier, len(ks) + across)


ROWS = 4
STRIP = 512
DMA = pltpu.SemaphoreType.DMA
SEMS = dict(
    xl=DMA((ROWS,)), wl=DMA((4,)), w1=DMA((2, 4, 3)), wz=DMA((2, 2)), wy=DMA((2, 2, 2)), wx=DMA((2, 2, 4)), a2=DMA((2, ROWS)), a1=DMA((2, ROWS)),
    af=DMA((2, ROWS)), kv=DMA((2, 3, 4)), o1=DMA((2, 5)), o3=DMA((2, 4)), ox=DMA((2, 7)), od=DMA((2, 2, 8)), ol=DMA, back=DMA((2, 3)),
    bl=DMA,
)


def layer(x_ref, gain_ref, wq_ref, wk_ref, wv_ref, wo_ref, freq_ref, seen_ref, wide_ref,
          x_s, cos_s, sin_s, a_s, w_s, q_s, kv_s, got, top_s, mix_s, out_s, gap_s, *sems):
    sem = dict(zip(SEMS, sems))
    s, d = lax.axis_index("sp"), lax.axis_index("dp")
    other = 1 - d
    g, zh, y = lax.rem(s, 4), lax.rem(lax.div(s, 4), 2), lax.div(s, 8)
    own = x_ref.shape[0]
    r = wk_ref.shape[0]
    e = HEAD**-0.5 * LOG2E
    sends = []

    def send(src, dst, pair, at, to, when=None):
        copy = pltpu.make_async_remote_copy(src_ref=src, dst_ref=dst, send_sem=pair.at[(0, *at)], recv_sem=pair.at[(1, *at)], device_id=to,
                                            device_id_type=MESH)
        if when is None:
            copy.start()
        else:
            pl.when(when)(copy.start)
        sends.append((copy, when))

    def arrived(dst, pair, at):
        pltpu.make_async_copy(dst, dst, pair.at[(1, *at)]).wait()

    def keep(src, dst, at):
        copy = pltpu.make_async_copy(src, dst, at)
        copy.start()
        return copy

    sp = lambda k: {"sp": flip(s, k)}
    across = {"dp": other}
    meet(s, d, (1, 2, 3, 4, 8), True)

    def head(part, g):
        if part < 2:
            return (wk_ref, wv_ref)[part].at[:, pl.ds(pl.multiple_of(g * HEAD, HEAD), HEAD)]
        return wq_ref.at[:, pl.ds(pl.multiple_of(g * 2 * HEAD + (part - 2) * HEAD, HEAD), HEAD)]

    def rows_of(part, t, n=1):
        return w_s.at[part // 2, pl.ds(pl.multiple_of(t * r, 32), n * r), pl.ds(part % 2 * HEAD, HEAD)]

    def mine(group, k):
        return w_s.at[group, pl.ds(pl.multiple_of(lax.div(flip(s, 4 * k), 4) * (4 * r), 128), 4 * r), pl.ds(pl.multiple_of(d * HEAD, HEAD), HEAD)]

    def theirs(group, k):
        return w_s.at[group, pl.ds(pl.multiple_of(lax.div(flip(s, 4 * k), 4) * (4 * r), 128), 4 * r), pl.ds(pl.multiple_of(other * HEAD, HEAD), HEAD)]

    loads = [keep(x_ref.at[pl.ds(i * (own // ROWS), own // ROWS)], x_s.at[pl.ds(i * (own // ROWS), own // ROWS)], sem["xl"].at[i]) for i in range(ROWS)]
    def first_stage(part, m):
        return pltpu.make_async_remote_copy(src_ref=head(part, flip(g, m)), dst_ref=rows_of(part, s), send_sem=sem["w1"].at[0, part, m - 1],
                                            recv_sem=sem["w1"].at[1, part, m - 1], device_id=sp(m), device_id_type=MESH)

    for group in (0, 1):
        for m in (2, 3):
            for i in (0, 1):
                @pl.when(d == i)
                def _():
                    first_stage(2 * group + i, m).start()
        for part in (2 * group, 2 * group + 1):
            first_stage(part, 1).start()
    kept = [keep(head(part, g), rows_of(part, s), sem["wl"].at[part]) for part in range(4)]
    kept_o = keep(wo_ref, wide_ref.at[pl.ds(pl.multiple_of(s * wo_ref.shape[0], 128), wo_ref.shape[0])], sem["ol"])

    n = own // ROWS
    gain = gain_ref[...].astype(jnp.float32)
    slot = lambda t, i=0, n=own: a_s.at[pl.ds(pl.multiple_of(t * own + i * n, n), n)]
    for i in range(ROWS):
        loads[i].wait()
        wide = x_s[i * n : (i + 1) * n, :].astype(jnp.float32)
        scale = lax.rsqrt(jnp.mean(wide * wide, -1, keepdims=True) + 1e-6)
        a_s[pl.ds(pl.multiple_of(g * own + i * n, n), n), :] = (wide * scale * gain).astype(jnp.bfloat16)
    gap_s[...] = lax.broadcasted_iota(jnp.int32, gap_s.shape, 1) - lax.broadcasted_iota(jnp.int32, gap_s.shape, 0)
    top_s[...] = jnp.full(top_s.shape, NEG, jnp.float32)
    mix_s[...] = jnp.zeros(mix_s.shape, jnp.float32)
    for i in range(ROWS):
        send(slot(g, i, n), slot(g, i, n), sem["a1"], (i,), sp(1))
    for copy in kept:
        copy.wait()

    def near(group, h):
        return w_s.at[group, pl.ds(pl.multiple_of(lax.div(flip(s, 2), 2) * (2 * r), 64), 2 * r), pl.ds(pl.multiple_of(h * HEAD, HEAD), HEAD)]

    def from_cluster(group):
        for part in (2 * group, 2 * group + 1):
            arrived(rows_of(part, flip(s, 1)), sem["w1"], (part, 0))
        for i in (0, 1):
            @pl.when(d == i)
            def _():
                for m in (2, 3):
                    arrived(rows_of(2 * group + i, flip(s, m)), sem["w1"], (2 * group + i, m - 1))

    def to_neighbour(i):
        send(slot(g, i, n), slot(g, i, n), sem["a2"], (i,), sp(2))

    for group in (0, 1):
        from_cluster(group)
        send(mine(group, 0), mine(group, 0), sem["wz"], (group,), sp(4))
        send(mine(group, 0), mine(group, 0), sem["wy"], (group, 0), sp(8))
        send(near(group, d), near(group, d), sem["wx"], (group, 3), across)
        if group == 0:
            to_neighbour(0)
            to_neighbour(1)

    orows, ocols = wo_ref.shape[0], wo_ref.shape[1] // 2
    half = lambda t, h: wide_ref.at[pl.ds(pl.multiple_of(flip(s, t) * orows, 128), orows), pl.ds(pl.multiple_of(h * ocols, 128), ocols)]
    EVEN = (0, 2, 4, 6, 8, 10, 12, 14)
    kept_o.wait()
    inner = lax.rem(lax.div(s, 2), 2) + zh == 1
    soon = inner & (zh == 0)
    to_neighbour(2)
    to_neighbour(3)
    send(half(0, d), half(0, d), sem["o1"], (0,), sp(2))
    send(half(0, d), half(0, d), sem["o1"], (1,), sp(6), inner)

    def o_on(i, to_y=False):
        k = EVEN[i]
        if to_y:
            send(half(k, d), half(k, d), sem["o3"], (i,), sp(8))
        if i:
            send(half(k, d), half(k, d), sem["ox"], (i - 1,), across)
        send(half(k, d), half(k, d), sem["od"], (0, i), sp(1))

    o_on(0, True)

    for i in range(4):
        spot = (lax.div(s, 4) * 4 + i) * own + lax.broadcasted_iota(jnp.int32, (own, HEAD // 2), 0)
        angle = spot.astype(jnp.float32) * freq_ref[...]
        cos_s[i * own : (i + 1) * own, :] = jnp.cos(angle)
        sin_s[i * own : (i + 1) * own, :] = jnp.sin(angle)

    def pass_y(group):
        arrived(mine(group, 2), sem["wy"], (group, 0))
        send(mine(group, 2), mine(group, 2), sem["wx"], (group, 0), across)

    def pass_z(group):
        arrived(mine(group, 1), sem["wz"], (group,))
        send(mine(group, 1), mine(group, 1), sem["wy"], (group, 1), sp(8))
        send(mine(group, 1), mine(group, 1), sem["wx"], (group, 1), across)
        arrived(mine(group, 3), sem["wy"], (group, 1))
        send(mine(group, 3), mine(group, 3), sem["wx"], (group, 2), across)

    def complete(group):
        for i, k in enumerate((2, 1, 3)):
            arrived(theirs(group, k), sem["wx"], (group, i))
        arrived(near(group, other), sem["wx"], (group, 3))

    place = lambda c: lax.rem(lax.div(g, 2) * 2 + c, 4)
    rows = lambda c: pl.ds(pl.multiple_of(place(c) * own, own), own)

    def turn(t, at):
        half = HEAD // 2
        t = t.astype(jnp.bfloat16).astype(jnp.float32)
        a, b, cos, sin = t[:, :half], t[:, half:], cos_s[at, :], sin_s[at, :]
        return (a * cos - b * sin).astype(jnp.bfloat16), (b * cos + a * sin).astype(jnp.bfloat16)

    def project(group, c):
        at = rows(c)
        half = HEAD // 2
        t = _dot(a_s[at, :], w_s[group], 1, 0)
        into = (kv_s, q_s)[group]
        into[at, :half], into[at, half:HEAD] = turn(t[:, :HEAD], at)
        if group == 0:
            into[at, HEAD:] = t[:, HEAD:].astype(jnp.bfloat16)
        else:
            into[at, HEAD : HEAD + half], into[at, HEAD + half :] = turn(t[:, HEAD:], at)

    to_z = (y == 0) | (zh == 0)
    from_z = (y == 0) | (zh == 1)

    def exchange(kind, c, src, k):
        return pltpu.make_async_remote_copy(src_ref=src.at[rows(c)], dst_ref=got.at[kind, rows(c)], send_sem=sem["kv"].at[0, kind, c],
                                            recv_sem=sem["kv"].at[1, kind, c], device_id=sp(k), device_id_type=MESH)

    def share_z(c):
        @pl.when(to_z)
        def _():
            exchange(1, c, kv_s, 4).start()

    def share_y(c):
        @pl.when(y == 0)
        def _():
            exchange(0, c, kv_s, 8).start()

    def forward(c):
        @pl.when(y == 0)
        def _():
            here = got.at[1, rows(c)]
            pltpu.make_async_copy(here, here, sem["kv"].at[1, 1, c]).wait()
            exchange(2, c, got.at[1], 8).start()

    def early(c, _):
        project(0, c)
        share_y(c)
        pl.when(soon)(lambda: share_z(c))

    def late(c, _):
        project(0, c)
        share_z(c)
        share_y(c)

    def queries(c, _):
        project(1, c)

    def relay(i):
        arrived(slot(flip(g, 2), i, n), sem["a2"], (i,))
        send(slot(flip(g, 2), i, n), slot(flip(g, 2), i, n), sem["af"], (i,), sp(1))

    pass_y(0)
    pass_z(0)
    for i in range(ROWS):
        arrived(slot(flip(g, 1), i, n), sem["a1"], (i,))
    complete(0)
    lax.fori_loop(0, 2, early, None)
    pass_y(1)
    pass_z(1)
    arrived(half(8, d), sem["o3"], (0,))
    o_on(4)
    for i in range(ROWS):
        relay(i)

    @pl.when(jnp.logical_not(soon))
    def _():
        share_z(0)
        share_z(1)

    arrived(half(2, d), sem["o1"], (0,))
    send(half(2, d), half(2, d), sem["o1"], (2,), sp(6), inner)
    o_on(1, True)
    for i in range(ROWS):
        arrived(slot(flip(g, 3), i, n), sem["af"], (i,))
    lax.fori_loop(2, 4, late, None)
    for i, k in enumerate((6, 4)):
        pl.when(inner)(functools.partial(arrived, half(k, d), sem["o1"], (1 + i,)))
        send(half(k, d), half(k, d), sem["o1"], (3 + i,), sp(2), inner)
        pl.when(jnp.logical_not(inner))(functools.partial(arrived, half(10 - k, d), sem["o1"], (3 + i,)))
    o_on(2, True)
    o_on(3, True)
    complete(1)
    lax.fori_loop(0, 4, queries, None)
    forward(0)
    forward(1)

    ones = jnp.ones((8, own), jnp.bfloat16)
    def block(keys, values, first=None):
        pieces = [(i, h) for i in range(first or 0, 4) for h in range(2)]
        scores = [_dot(keys, q_s[i * STRIP : (i + 1) * STRIP, h * HEAD : (h + 1) * HEAD], 1, 1) for i, h in pieces]
        weights, keeps = [], []
        for (i, h), sc in zip(pieces, scores):
            cols = slice((2 * i + h) * STRIP, (2 * i + h + 1) * STRIP)
            if i == first:
                sc = jnp.where(gap_s[...] >= 0, sc, HIDDEN)
            old = top_s[:, cols]
            top = jnp.maximum(old, sc.max(axis=0, keepdims=True))
            top_s[:, cols] = top
            weights.append(jnp.exp2((sc - top) * e).astype(jnp.bfloat16))
            keeps.append(jnp.exp2((old - top) * e))
        turned_values = jnp.concatenate([values.T, ones], axis=0)
        for (i, h), p, keep in zip(pieces, weights, keeps):
            cols = slice((2 * i + h) * STRIP, (2 * i + h + 1) * STRIP)
            mix_s[:, cols] = mix_s[:, cols] * keep + _dot(turned_values, p, 1, 0)

    for i in range(4):
        block(kv_s[i * own : (i + 1) * own, :HEAD], kv_s[i * own : (i + 1) * own, HEAD:], i)

    def visit(t, _):
        late, kind, c = lax.div(t, 6), lax.rem(lax.div(t, 2), 3), lax.rem(t, 2)
        c = c + 2 * late
        comes = jnp.where(kind == 1, ((y == 0) & (late == 1)) | ((y == 1) & (zh == 1)), y == 1)
        wanted = jnp.where(kind == 1, zh == 1, y == 1)

        @pl.when(comes)
        def _():
            here = got.at[kind, rows(c)]
            pltpu.make_async_copy(here, here, sem["kv"].at[1, kind, c]).wait()

        @pl.when((kind == 1) & (y == 0) & (late == 1))
        def _():
            exchange(2, c, got.at[1], 8).start()

        @pl.when(wanted)
        def _():
            block(got[kind, rows(c), :HEAD], got[kind, rows(c), HEAD:])

    lax.fori_loop(0, 6, visit, None)
    for i in (5, 6, 7):
        arrived(half(EVEN[i], d), sem["o3"], (i - 4,))
        o_on(i)
    lax.fori_loop(6, 12, visit, None)

    for at in range(8):
        i, h, cols = at // 2, at % 2, slice(at * STRIP, (at + 1) * STRIP)
        out = mix_s[:HEAD, cols] * (1 / mix_s[HEAD : HEAD + 1, cols])
        out_s[i, :, h * HEAD : (h + 1) * HEAD] = out.T.astype(jnp.bfloat16)
    columns = lambda t: seen_ref.at[:, pl.ds(pl.multiple_of(t * 2 * HEAD, 2 * HEAD), 2 * HEAD)]
    for m in (2, 3, 1):
        send(out_s.at[flip(g, m)], columns(g), sem["back"], (m - 1,), sp(m))
    kept_b = keep(out_s.at[g], columns(g), sem["bl"])
    send(half(0, other), half(0, other), sem["od"], (1, 0), sp(1))
    for i in range(1, 8):
        arrived(half(EVEN[i], other), sem["ox"], (i - 1,))
        send(half(EVEN[i], other), half(EVEN[i], other), sem["od"], (1, i), sp(1))
    for i in range(8):
        arrived(half(EVEN[i] + 1, d), sem["od"], (0, i))
        arrived(half(EVEN[i] + 1, other), sem["od"], (1, i))
    for m in (1, 2, 3):
        arrived(columns(flip(g, m)), sem["back"], (m - 1,))
    kept_b.wait()
    for copy, when in sends:
        if when is None:
            copy.wait_send()
        else:
            pl.when(when)(copy.wait_send)
    for group in (0, 1):
        for i in (0, 1):
            @pl.when(d == i)
            def _():
                for m in (2, 3):
                    first_stage(2 * group + i, m).wait_send()
        for part in (2 * group, 2 * group + 1):
            first_stage(part, 1).wait_send()

    for c in range(4):
        @pl.when(to_z)
        def _():
            exchange(1, c, kv_s, 4).wait_send()

        @pl.when(y == 0)
        def _():
            exchange(0, c, kv_s, 8).wait_send()
            exchange(2, c, got.at[1], 8).wait_send()


def attended(x, gain, wq, wk, wv, wo, freq):
    own, width = x.shape
    bf16, f32 = jnp.bfloat16, jnp.float32
    vmem, hbm = pl.BlockSpec(memory_space=pltpu.VMEM), pl.BlockSpec(memory_space=pl.ANY)
    return pl.pallas_call(
        layer,
        out_shape=[jax.ShapeDtypeStruct((own, 4 * 2 * HEAD), bf16), jax.ShapeDtypeStruct((16 * wo.shape[0], wo.shape[1]), bf16)],
        in_specs=[hbm, vmem, hbm, hbm, hbm, vmem, vmem],
        out_specs=[hbm] * 2,
        scratch_shapes=[
            pltpu.VMEM((own, width), bf16),
            pltpu.VMEM((4 * own, HEAD // 2), f32),
            pltpu.VMEM((4 * own, HEAD // 2), f32),
            pltpu.VMEM((4 * own, width), bf16),
            pltpu.VMEM((2, 16 * wk.shape[0], 2 * HEAD), bf16),
            pltpu.VMEM((4 * own, 2 * HEAD), bf16),
            pltpu.VMEM((4 * own, 2 * HEAD), bf16),
            pltpu.VMEM((3, 4 * own, 2 * HEAD), bf16),
            pltpu.VMEM((1, 8 * own), f32),
            pltpu.VMEM((HEAD + 8, 8 * own), f32),
            pltpu.VMEM((4, own, 2 * HEAD), bf16),
            pltpu.VMEM((own, STRIP), jnp.int32),
            *SEMS.values(),
        ],
        compiler_params=pltpu.CompilerParams(collective_id=0, has_side_effects=True, vmem_limit_bytes=VMEM),
    )(x, gain, wq, wk, wv, wo, freq)


def solution(mesh):
    def step(x, gain, wq, wk, wv, wo):
        half = HEAD // 2
        freq = THETA ** (-jnp.arange(half, dtype=jnp.float32) / half)
        seen, wide = attended(x, gain, wq, wk, wv, wo, freq[None])
        y = jnp.dot(seen, wide, preferred_element_type=jnp.float32)
        return (x.astype(jnp.float32) + y).astype(jnp.bfloat16)

    tokens, whole = P(("dp", "sp"), None), P("sp", None)
    return jax.shard_map(
        step,
        mesh=mesh,
        in_specs=(tokens, P(None), whole, whole, whole, whole),
        out_specs=tokens,
        check_vma=False,
    )
```

```python
import functools

import jax
import jax.numpy as jnp
from jax import lax
from jax.experimental import pallas as pl
from jax.experimental.pallas import tpu as pltpu
from jax.sharding import PartitionSpec as P

NEG = -1e30
HIDDEN = 2 * NEG
LOG2E = 1.4426950408889634
VMEM = 63 * 2**20
HEAD = 256
THETA = 10000
MESH = pl.DeviceIdType.MESH


def _dot(a, b, ca, cb):
    return lax.dot_general(a, b, (((ca,), (cb,)), ((), ())), preferred_element_type=jnp.float32)


def flip(s, k):
    for bit in (1, 2, 4, 8):
        if k & bit:
            s = s + bit - 2 * bit * lax.rem(lax.div(s, bit), 2)
    return s


def meet(s, d, ks, across):
    barrier = pltpu.get_barrier_semaphore()
    for k in ks:
        pl.semaphore_signal(barrier, inc=1, device_id={"sp": flip(s, k)}, device_id_type=MESH)
    if across:
        pl.semaphore_signal(barrier, inc=1, device_id={"dp": 1 - d}, device_id_type=MESH)
    pl.semaphore_wait(barrier, len(ks) + across)


ROWS = 4
STRIP = 512
DMA = pltpu.SemaphoreType.DMA
SEMS = dict(
    xl=DMA((ROWS,)), wl=DMA((4,)), w1=DMA((2, 4, 3)), wz=DMA((2, 2)), wy=DMA((2, 2, 2)), wx=DMA((2, 2, 4)), a2=DMA((2, ROWS)), a1=DMA((2, ROWS)),
    af=DMA((2, ROWS)), kv=DMA((2, 3, 4)), o1=DMA((2, 5)), o3=DMA((2, 4)), ox=DMA((2, 7)), od=DMA((2, 2, 8)), ol=DMA, back=DMA((2, 3)),
    bl=DMA,
)


def layer(x_ref, gain_ref, wq_ref, wk_ref, wv_ref, wo_ref, freq_ref, seen_ref, wide_ref,
          x_s, cos_s, sin_s, a_s, w_s, q_s, kv_s, got, top_s, mix_s, out_s, gap_s, *sems):
    sem = dict(zip(SEMS, sems))
    s, d = lax.axis_index("sp"), lax.axis_index("dp")
    other = 1 - d
    g, zh, y = lax.rem(s, 4), lax.rem(lax.div(s, 4), 2), lax.div(s, 8)
    own = x_ref.shape[0]
    r = wk_ref.shape[0]
    e = HEAD**-0.5 * LOG2E
    sends = []

    def send(src, dst, pair, at, to, when=None):
        copy = pltpu.make_async_remote_copy(src_ref=src, dst_ref=dst, send_sem=pair.at[(0, *at)], recv_sem=pair.at[(1, *at)], device_id=to,
                                            device_id_type=MESH)
        if when is None:
            copy.start()
        else:
            pl.when(when)(copy.start)
        sends.append((copy, when))

    def arrived(dst, pair, at):
        pltpu.make_async_copy(dst, dst, pair.at[(1, *at)]).wait()

    def keep(src, dst, at):
        copy = pltpu.make_async_copy(src, dst, at)
        copy.start()
        return copy

    sp = lambda k: {"sp": flip(s, k)}
    across = {"dp": other}
    meet(s, d, (1, 2, 3, 4, 8), True)

    def head(part, g):
        if part < 2:
            return (wk_ref, wv_ref)[part].at[:, pl.ds(pl.multiple_of(g * HEAD, HEAD), HEAD)]
        return wq_ref.at[:, pl.ds(pl.multiple_of(g * 2 * HEAD + (part - 2) * HEAD, HEAD), HEAD)]

    def rows_of(part, t, n=1):
        return w_s.at[part // 2, pl.ds(pl.multiple_of(t * r, 32), n * r), pl.ds(part % 2 * HEAD, HEAD)]

    def mine(group, k):
        return w_s.at[group, pl.ds(pl.multiple_of(lax.div(flip(s, 4 * k), 4) * (4 * r), 128), 4 * r), pl.ds(pl.multiple_of(d * HEAD, HEAD), HEAD)]

    def theirs(group, k):
        return w_s.at[group, pl.ds(pl.multiple_of(lax.div(flip(s, 4 * k), 4) * (4 * r), 128), 4 * r), pl.ds(pl.multiple_of(other * HEAD, HEAD), HEAD)]

    loads = [keep(x_ref.at[pl.ds(i * (own // ROWS), own // ROWS)], x_s.at[pl.ds(i * (own // ROWS), own // ROWS)], sem["xl"].at[i]) for i in range(ROWS)]
    def first_stage(part, m):
        return pltpu.make_async_remote_copy(src_ref=head(part, flip(g, m)), dst_ref=rows_of(part, s), send_sem=sem["w1"].at[0, part, m - 1],
                                            recv_sem=sem["w1"].at[1, part, m - 1], device_id=sp(m), device_id_type=MESH)

    for group in (0, 1):
        for m in (2, 3):
            for i in (0, 1):
                @pl.when(d == i)
                def _():
                    first_stage(2 * group + i, m).start()
        for part in (2 * group, 2 * group + 1):
            first_stage(part, 1).start()
    kept = [keep(head(part, g), rows_of(part, s), sem["wl"].at[part]) for part in range(4)]
    kept_o = keep(wo_ref, wide_ref.at[pl.ds(pl.multiple_of(s * wo_ref.shape[0], 128), wo_ref.shape[0])], sem["ol"])

    n = own // ROWS
    gain = gain_ref[...].astype(jnp.float32)
    slot = lambda t, i=0, n=own: a_s.at[pl.ds(pl.multiple_of(t * own + i * n, n), n)]
    for i in range(ROWS):
        loads[i].wait()
        wide = x_s[i * n : (i + 1) * n, :].astype(jnp.float32)
        scale = lax.rsqrt(jnp.mean(wide * wide, -1, keepdims=True) + 1e-6)
        a_s[pl.ds(pl.multiple_of(g * own + i * n, n), n), :] = (wide * scale * gain).astype(jnp.bfloat16)
    gap_s[...] = lax.broadcasted_iota(jnp.int32, gap_s.shape, 1) - lax.broadcasted_iota(jnp.int32, gap_s.shape, 0)
    top_s[...] = jnp.full(top_s.shape, NEG, jnp.float32)
    mix_s[...] = jnp.zeros(mix_s.shape, jnp.float32)
    for i in range(ROWS):
        send(slot(g, i, n), slot(g, i, n), sem["a1"], (i,), sp(1))
    for copy in kept:
        copy.wait()

    def near(group, h):
        return w_s.at[group, pl.ds(pl.multiple_of(lax.div(flip(s, 2), 2) * (2 * r), 64), 2 * r), pl.ds(pl.multiple_of(h * HEAD, HEAD), HEAD)]

    def from_cluster(group):
        for part in (2 * group, 2 * group + 1):
            arrived(rows_of(part, flip(s, 1)), sem["w1"], (part, 0))
        for i in (0, 1):
            @pl.when(d == i)
            def _():
                for m in (2, 3):
                    arrived(rows_of(2 * group + i, flip(s, m)), sem["w1"], (2 * group + i, m - 1))

    def to_neighbour(i):
        send(slot(g, i, n), slot(g, i, n), sem["a2"], (i,), sp(2))

    for group in (0, 1):
        from_cluster(group)
        send(mine(group, 0), mine(group, 0), sem["wz"], (group,), sp(4))
        send(mine(group, 0), mine(group, 0), sem["wy"], (group, 0), sp(8))
        send(near(group, d), near(group, d), sem["wx"], (group, 3), across)
        if group == 0:
            to_neighbour(0)
            to_neighbour(1)

    orows, ocols = wo_ref.shape[0], wo_ref.shape[1] // 2
    half = lambda t, h: wide_ref.at[pl.ds(pl.multiple_of(flip(s, t) * orows, 128), orows), pl.ds(pl.multiple_of(h * ocols, 128), ocols)]
    EVEN = (0, 2, 4, 6, 8, 10, 12, 14)
    kept_o.wait()
    inner = lax.rem(lax.div(s, 2), 2) + zh == 1
    send(half(0, d), half(0, d), sem["o1"], (0,), sp(2))
    send(half(0, d), half(0, d), sem["o1"], (1,), sp(6), inner)
    to_neighbour(2)
    to_neighbour(3)

    def o_on(i, to_y=False):
        k = EVEN[i]
        if to_y:
            send(half(k, d), half(k, d), sem["o3"], (i,), sp(8))
        if i:
            send(half(k, d), half(k, d), sem["ox"], (i - 1,), across)
        send(half(k, d), half(k, d), sem["od"], (0, i), sp(1))

    o_on(0, True)

    for i in range(4):
        spot = (lax.div(s, 4) * 4 + i) * own + lax.broadcasted_iota(jnp.int32, (own, HEAD // 2), 0)
        angle = spot.astype(jnp.float32) * freq_ref[...]
        cos_s[i * own : (i + 1) * own, :] = jnp.cos(angle)
        sin_s[i * own : (i + 1) * own, :] = jnp.sin(angle)

    def pass_y(group):
        arrived(mine(group, 2), sem["wy"], (group, 0))
        send(mine(group, 2), mine(group, 2), sem["wx"], (group, 0), across)

    def pass_z(group):
        arrived(mine(group, 1), sem["wz"], (group,))
        send(mine(group, 1), mine(group, 1), sem["wy"], (group, 1), sp(8))
        send(mine(group, 1), mine(group, 1), sem["wx"], (group, 1), across)
        arrived(mine(group, 3), sem["wy"], (group, 1))
        send(mine(group, 3), mine(group, 3), sem["wx"], (group, 2), across)

    def complete(group):
        for i, k in enumerate((2, 1, 3)):
            arrived(theirs(group, k), sem["wx"], (group, i))
        arrived(near(group, other), sem["wx"], (group, 3))

    place = lambda c: lax.rem(lax.div(g, 2) * 2 + c, 4)
    rows = lambda c: pl.ds(pl.multiple_of(place(c) * own, own), own)

    def turn(t, at):
        half = HEAD // 2
        t = t.astype(jnp.bfloat16).astype(jnp.float32)
        a, b, cos, sin = t[:, :half], t[:, half:], cos_s[at, :], sin_s[at, :]
        return (a * cos - b * sin).astype(jnp.bfloat16), (b * cos + a * sin).astype(jnp.bfloat16)

    def project(group, c):
        at = rows(c)
        half = HEAD // 2
        t = _dot(a_s[at, :], w_s[group], 1, 0)
        into = (kv_s, q_s)[group]
        into[at, :half], into[at, half:HEAD] = turn(t[:, :HEAD], at)
        if group == 0:
            into[at, HEAD:] = t[:, HEAD:].astype(jnp.bfloat16)
        else:
            into[at, HEAD : HEAD + half], into[at, HEAD + half :] = turn(t[:, HEAD:], at)

    to_z = (y == 0) | (zh == 0)
    from_z = (y == 0) | (zh == 1)

    def exchange(kind, c, src, k):
        return pltpu.make_async_remote_copy(src_ref=src.at[rows(c)], dst_ref=got.at[kind, rows(c)], send_sem=sem["kv"].at[0, kind, c],
                                            recv_sem=sem["kv"].at[1, kind, c], device_id=sp(k), device_id_type=MESH)

    def share_z(c):
        @pl.when(to_z)
        def _():
            exchange(1, c, kv_s, 4).start()

    def share_y(c):
        @pl.when(y == 0)
        def _():
            exchange(0, c, kv_s, 8).start()

    def forward(c):
        @pl.when(y == 0)
        def _():
            here = got.at[1, rows(c)]
            pltpu.make_async_copy(here, here, sem["kv"].at[1, 1, c]).wait()
            exchange(2, c, got.at[1], 8).start()

    def early(c, _):
        project(0, c)
        share_y(c)

    def late(c, _):
        project(0, c)
        share_z(c)
        share_y(c)

    def queries(c, _):
        project(1, c)

    def relay(i):
        arrived(slot(flip(g, 2), i, n), sem["a2"], (i,))
        send(slot(flip(g, 2), i, n), slot(flip(g, 2), i, n), sem["af"], (i,), sp(1))

    pass_y(0)
    pass_z(0)
    arrived(half(2, d), sem["o1"], (0,))
    send(half(2, d), half(2, d), sem["o1"], (2,), sp(6), inner)
    o_on(1, True)
    for i in range(ROWS):
        arrived(slot(flip(g, 1), i, n), sem["a1"], (i,))
    complete(0)
    lax.fori_loop(0, 2, early, None)
    pass_y(1)
    pass_z(1)
    arrived(half(8, d), sem["o3"], (0,))
    o_on(4)
    for i in range(ROWS):
        relay(i)

    share_z(0)
    share_z(1)

    for i in range(ROWS):
        arrived(slot(flip(g, 3), i, n), sem["af"], (i,))
    lax.fori_loop(2, 4, late, None)
    for i, k in enumerate((6, 4)):
        pl.when(inner)(functools.partial(arrived, half(k, d), sem["o1"], (1 + i,)))
        send(half(k, d), half(k, d), sem["o1"], (3 + i,), sp(2), inner)
        pl.when(jnp.logical_not(inner))(functools.partial(arrived, half(10 - k, d), sem["o1"], (3 + i,)))
    o_on(2, True)
    o_on(3, True)
    complete(1)
    lax.fori_loop(0, 4, queries, None)
    forward(0)
    forward(1)

    ones = jnp.ones((8, own), jnp.bfloat16)
    def block(keys, values, first=None):
        pieces = [(i, h) for i in range(first or 0, 4) for h in range(2)]
        scores = [_dot(keys, q_s[i * STRIP : (i + 1) * STRIP, h * HEAD : (h + 1) * HEAD], 1, 1) for i, h in pieces]
        weights, keeps = [], []
        for (i, h), sc in zip(pieces, scores):
            cols = slice((2 * i + h) * STRIP, (2 * i + h + 1) * STRIP)
            if i == first:
                sc = jnp.where(gap_s[...] >= 0, sc, HIDDEN)
            old = top_s[:, cols]
            top = jnp.maximum(old, sc.max(axis=0, keepdims=True))
            top_s[:, cols] = top
            weights.append(jnp.exp2((sc - top) * e).astype(jnp.bfloat16))
            keeps.append(jnp.exp2((old - top) * e))
        turned_values = jnp.concatenate([values.T, ones], axis=0)
        for (i, h), p, keep in zip(pieces, weights, keeps):
            cols = slice((2 * i + h) * STRIP, (2 * i + h + 1) * STRIP)
            mix_s[:, cols] = mix_s[:, cols] * keep + _dot(turned_values, p, 1, 0)

    for i in range(4):
        block(kv_s[i * own : (i + 1) * own, :HEAD], kv_s[i * own : (i + 1) * own, HEAD:], i)

    def visit(t, _):
        late, kind, c = lax.div(t, 6), lax.rem(lax.div(t, 2), 3), lax.rem(t, 2)
        c = c + 2 * late
        comes = jnp.where(kind == 1, ((y == 0) & (late == 1)) | ((y == 1) & (zh == 1)), y == 1)
        wanted = jnp.where(kind == 1, zh == 1, y == 1)

        @pl.when(comes)
        def _():
            here = got.at[kind, rows(c)]
            pltpu.make_async_copy(here, here, sem["kv"].at[1, kind, c]).wait()

        @pl.when((kind == 1) & (y == 0) & (late == 1))
        def _():
            exchange(2, c, got.at[1], 8).start()

        @pl.when(wanted)
        def _():
            block(got[kind, rows(c), :HEAD], got[kind, rows(c), HEAD:])

    lax.fori_loop(0, 6, visit, None)
    for i in (5, 6, 7):
        arrived(half(EVEN[i], d), sem["o3"], (i - 4,))
        o_on(i)
    lax.fori_loop(6, 12, visit, None)

    for at in range(8):
        i, h, cols = at // 2, at % 2, slice(at * STRIP, (at + 1) * STRIP)
        out = mix_s[:HEAD, cols] * (1 / mix_s[HEAD : HEAD + 1, cols])
        out_s[i, :, h * HEAD : (h + 1) * HEAD] = out.T.astype(jnp.bfloat16)
    columns = lambda t: seen_ref.at[:, pl.ds(pl.multiple_of(t * 2 * HEAD, 2 * HEAD), 2 * HEAD)]
    for m in (2, 3, 1):
        send(out_s.at[flip(g, m)], columns(g), sem["back"], (m - 1,), sp(m))
    kept_b = keep(out_s.at[g], columns(g), sem["bl"])
    send(half(0, other), half(0, other), sem["od"], (1, 0), sp(1))
    for i in range(1, 8):
        arrived(half(EVEN[i], other), sem["ox"], (i - 1,))
        send(half(EVEN[i], other), half(EVEN[i], other), sem["od"], (1, i), sp(1))
    for i in range(8):
        arrived(half(EVEN[i] + 1, d), sem["od"], (0, i))
        arrived(half(EVEN[i] + 1, other), sem["od"], (1, i))
    for m in (1, 2, 3):
        arrived(columns(flip(g, m)), sem["back"], (m - 1,))
    kept_b.wait()
    for copy, when in sends:
        if when is None:
            copy.wait_send()
        else:
            pl.when(when)(copy.wait_send)
    for group in (0, 1):
        for i in (0, 1):
            @pl.when(d == i)
            def _():
                for m in (2, 3):
                    first_stage(2 * group + i, m).wait_send()
        for part in (2 * group, 2 * group + 1):
            first_stage(part, 1).wait_send()

    for c in range(4):
        @pl.when(to_z)
        def _():
            exchange(1, c, kv_s, 4).wait_send()

        @pl.when(y == 0)
        def _():
            exchange(0, c, kv_s, 8).wait_send()
            exchange(2, c, got.at[1], 8).wait_send()


def attended(x, gain, wq, wk, wv, wo, freq):
    own, width = x.shape
    bf16, f32 = jnp.bfloat16, jnp.float32
    vmem, hbm = pl.BlockSpec(memory_space=pltpu.VMEM), pl.BlockSpec(memory_space=pl.ANY)
    return pl.pallas_call(
        layer,
        out_shape=[jax.ShapeDtypeStruct((own, 4 * 2 * HEAD), bf16), jax.ShapeDtypeStruct((16 * wo.shape[0], wo.shape[1]), bf16)],
        in_specs=[hbm, vmem, hbm, hbm, hbm, vmem, vmem],
        out_specs=[hbm] * 2,
        scratch_shapes=[
            pltpu.VMEM((own, width), bf16),
            pltpu.VMEM((4 * own, HEAD // 2), f32),
            pltpu.VMEM((4 * own, HEAD // 2), f32),
            pltpu.VMEM((4 * own, width), bf16),
            pltpu.VMEM((2, 16 * wk.shape[0], 2 * HEAD), bf16),
            pltpu.VMEM((4 * own, 2 * HEAD), bf16),
            pltpu.VMEM((4 * own, 2 * HEAD), bf16),
            pltpu.VMEM((3, 4 * own, 2 * HEAD), bf16),
            pltpu.VMEM((1, 8 * own), f32),
            pltpu.VMEM((HEAD + 8, 8 * own), f32),
            pltpu.VMEM((4, own, 2 * HEAD), bf16),
            pltpu.VMEM((own, STRIP), jnp.int32),
            *SEMS.values(),
        ],
        compiler_params=pltpu.CompilerParams(collective_id=0, has_side_effects=True, vmem_limit_bytes=VMEM),
    )(x, gain, wq, wk, wv, wo, freq)


def solution(mesh):
    def step(x, gain, wq, wk, wv, wo):
        half = HEAD // 2
        freq = THETA ** (-jnp.arange(half, dtype=jnp.float32) / half)
        seen, wide = attended(x, gain, wq, wk, wv, wo, freq[None])
        y = jnp.dot(seen, wide, preferred_element_type=jnp.float32)
        return (x.astype(jnp.float32) + y).astype(jnp.bfloat16)

    tokens, whole = P(("dp", "sp"), None), P("sp", None)
    return jax.shard_map(
        step,
        mesh=mesh,
        in_specs=(tokens, P(None), whole, whole, whole, whole),
        out_specs=tokens,
        check_vma=False,
    )
```

```python
import functools

import jax
import jax.numpy as jnp
from jax import lax
from jax.experimental import pallas as pl
from jax.experimental.pallas import tpu as pltpu
from jax.sharding import PartitionSpec as P

NEG = -1e30
HIDDEN = 2 * NEG
LOG2E = 1.4426950408889634
VMEM = 63 * 2**20
HEAD = 256
THETA = 10000
MESH = pl.DeviceIdType.MESH


def _dot(a, b, ca, cb):
    return lax.dot_general(a, b, (((ca,), (cb,)), ((), ())), preferred_element_type=jnp.float32)


def flip(s, k):
    for bit in (1, 2, 4, 8):
        if k & bit:
            s = s + bit - 2 * bit * lax.rem(lax.div(s, bit), 2)
    return s


def meet(s, d, ks, across):
    barrier = pltpu.get_barrier_semaphore()
    for k in ks:
        pl.semaphore_signal(barrier, inc=1, device_id={"sp": flip(s, k)}, device_id_type=MESH)
    if across:
        pl.semaphore_signal(barrier, inc=1, device_id={"dp": 1 - d}, device_id_type=MESH)
    pl.semaphore_wait(barrier, len(ks) + across)


ROWS = 4
STRIP = 512
DMA = pltpu.SemaphoreType.DMA
SEMS = dict(
    xl=DMA((ROWS,)), wl=DMA((4,)), w1=DMA((2, 4, 3)), wz=DMA((2, 2)), wy=DMA((2, 2, 2)), wx=DMA((2, 2, 4)), a2=DMA((2, ROWS)), a1=DMA((2, ROWS)),
    af=DMA((2, ROWS)), kv=DMA((2, 3, 4)), o1=DMA((2, 5)), o3=DMA((2, 4)), ox=DMA((2, 7)), od=DMA((2, 2, 8)), ol=DMA, back=DMA((2, 3)),
    bl=DMA,
)


def layer(x_ref, gain_ref, wq_ref, wk_ref, wv_ref, wo_ref, freq_ref, seen_ref, wide_ref,
          x_s, cos_s, sin_s, a_s, w_s, q_s, kv_s, got, top_s, mix_s, out_s, gap_s, *sems):
    sem = dict(zip(SEMS, sems))
    s, d = lax.axis_index("sp"), lax.axis_index("dp")
    other = 1 - d
    g, zh, y = lax.rem(s, 4), lax.rem(lax.div(s, 4), 2), lax.div(s, 8)
    own = x_ref.shape[0]
    r = wk_ref.shape[0]
    e = HEAD**-0.5 * LOG2E
    sends = []

    def send(src, dst, pair, at, to, when=None):
        copy = pltpu.make_async_remote_copy(src_ref=src, dst_ref=dst, send_sem=pair.at[(0, *at)], recv_sem=pair.at[(1, *at)], device_id=to,
                                            device_id_type=MESH)
        if when is None:
            copy.start()
        else:
            pl.when(when)(copy.start)
        sends.append((copy, when))

    def arrived(dst, pair, at):
        pltpu.make_async_copy(dst, dst, pair.at[(1, *at)]).wait()

    def keep(src, dst, at):
        copy = pltpu.make_async_copy(src, dst, at)
        copy.start()
        return copy

    sp = lambda k: {"sp": flip(s, k)}
    across = {"dp": other}
    meet(s, d, (1, 2, 3, 4, 8), True)

    def head(part, g):
        if part < 2:
            return (wk_ref, wv_ref)[part].at[:, pl.ds(pl.multiple_of(g * HEAD, HEAD), HEAD)]
        return wq_ref.at[:, pl.ds(pl.multiple_of(g * 2 * HEAD + (part - 2) * HEAD, HEAD), HEAD)]

    def rows_of(part, t, n=1):
        return w_s.at[part // 2, pl.ds(pl.multiple_of(t * r, 32), n * r), pl.ds(part % 2 * HEAD, HEAD)]

    def mine(group, k):
        return w_s.at[group, pl.ds(pl.multiple_of(lax.div(flip(s, 4 * k), 4) * (4 * r), 128), 4 * r), pl.ds(pl.multiple_of(d * HEAD, HEAD), HEAD)]

    def theirs(group, k):
        return w_s.at[group, pl.ds(pl.multiple_of(lax.div(flip(s, 4 * k), 4) * (4 * r), 128), 4 * r), pl.ds(pl.multiple_of(other * HEAD, HEAD), HEAD)]

    loads = [keep(x_ref.at[pl.ds(i * (own // ROWS), own // ROWS)], x_s.at[pl.ds(i * (own // ROWS), own // ROWS)], sem["xl"].at[i]) for i in range(ROWS)]
    def first_stage(part, m):
        return pltpu.make_async_remote_copy(src_ref=head(part, flip(g, m)), dst_ref=rows_of(part, s), send_sem=sem["w1"].at[0, part, m - 1],
                                            recv_sem=sem["w1"].at[1, part, m - 1], device_id=sp(m), device_id_type=MESH)

    for group in (0, 1):
        for m in (2, 3):
            for i in (0, 1):
                @pl.when(d == i)
                def _():
                    first_stage(2 * group + i, m).start()
        for part in (2 * group, 2 * group + 1):
            first_stage(part, 1).start()
    kept = [keep(head(part, g), rows_of(part, s), sem["wl"].at[part]) for part in range(4)]
    kept_o = keep(wo_ref, wide_ref.at[pl.ds(pl.multiple_of(s * wo_ref.shape[0], 128), wo_ref.shape[0])], sem["ol"])

    n = own // ROWS
    gain = gain_ref[...].astype(jnp.float32)
    slot = lambda t, i=0, n=own: a_s.at[pl.ds(pl.multiple_of(t * own + i * n, n), n)]
    for i in range(ROWS):
        loads[i].wait()
        wide = x_s[i * n : (i + 1) * n, :].astype(jnp.float32)
        scale = lax.rsqrt(jnp.mean(wide * wide, -1, keepdims=True) + 1e-6)
        a_s[pl.ds(pl.multiple_of(g * own + i * n, n), n), :] = (wide * scale * gain).astype(jnp.bfloat16)
    gap_s[...] = lax.broadcasted_iota(jnp.int32, gap_s.shape, 1) - lax.broadcasted_iota(jnp.int32, gap_s.shape, 0)
    top_s[...] = jnp.full(top_s.shape, NEG, jnp.float32)
    mix_s[...] = jnp.zeros(mix_s.shape, jnp.float32)
    for i in range(ROWS):
        send(slot(g, i, n), slot(g, i, n), sem["a1"], (i,), sp(1))
    for copy in kept:
        copy.wait()

    def near(group, h):
        return w_s.at[group, pl.ds(pl.multiple_of(lax.div(flip(s, 2), 2) * (2 * r), 64), 2 * r), pl.ds(pl.multiple_of(h * HEAD, HEAD), HEAD)]

    def from_cluster(group):
        for part in (2 * group, 2 * group + 1):
            arrived(rows_of(part, flip(s, 1)), sem["w1"], (part, 0))
        for i in (0, 1):
            @pl.when(d == i)
            def _():
                for m in (2, 3):
                    arrived(rows_of(2 * group + i, flip(s, m)), sem["w1"], (2 * group + i, m - 1))

    def to_neighbour(i):
        send(slot(g, i, n), slot(g, i, n), sem["a2"], (i,), sp(2))

    for group in (0, 1):
        from_cluster(group)
        send(mine(group, 0), mine(group, 0), sem["wz"], (group,), sp(4))
        send(mine(group, 0), mine(group, 0), sem["wy"], (group, 0), sp(8))
        send(near(group, d), near(group, d), sem["wx"], (group, 3), across)
        if group == 0:
            to_neighbour(0)
            to_neighbour(1)

    orows, ocols = wo_ref.shape[0], wo_ref.shape[1] // 2
    half = lambda t, h: wide_ref.at[pl.ds(pl.multiple_of(flip(s, t) * orows, 128), orows), pl.ds(pl.multiple_of(h * ocols, 128), ocols)]
    EVEN = (0, 2, 4, 6, 8, 10, 12, 14)
    kept_o.wait()
    inner = lax.rem(lax.div(s, 2), 2) + zh == 1
    send(half(0, d), half(0, d), sem["o1"], (0,), sp(2))
    send(half(0, d), half(0, d), sem["o1"], (1,), sp(6), inner)
    to_neighbour(2)
    to_neighbour(3)

    def o_on(i, to_y=False, when=None):
        k = EVEN[i]
        if to_y:
            send(half(k, d), half(k, d), sem["o3"], (i,), sp(8), when)
        if i:
            send(half(k, d), half(k, d), sem["ox"], (i - 1,), across, when)
        send(half(k, d), half(k, d), sem["od"], (0, i), sp(1), when)

    o_on(0, True)

    for i in range(4):
        spot = (lax.div(s, 4) * 4 + i) * own + lax.broadcasted_iota(jnp.int32, (own, HEAD // 2), 0)
        angle = spot.astype(jnp.float32) * freq_ref[...]
        cos_s[i * own : (i + 1) * own, :] = jnp.cos(angle)
        sin_s[i * own : (i + 1) * own, :] = jnp.sin(angle)

    def pass_y(group):
        arrived(mine(group, 2), sem["wy"], (group, 0))
        send(mine(group, 2), mine(group, 2), sem["wx"], (group, 0), across)

    def pass_z(group):
        arrived(mine(group, 1), sem["wz"], (group,))
        send(mine(group, 1), mine(group, 1), sem["wy"], (group, 1), sp(8))
        send(mine(group, 1), mine(group, 1), sem["wx"], (group, 1), across)
        arrived(mine(group, 3), sem["wy"], (group, 1))
        send(mine(group, 3), mine(group, 3), sem["wx"], (group, 2), across)

    def complete(group):
        for i, k in enumerate((2, 1, 3)):
            arrived(theirs(group, k), sem["wx"], (group, i))
        arrived(near(group, other), sem["wx"], (group, 3))

    place = lambda c: lax.rem(lax.div(g, 2) * 2 + c, 4)
    rows = lambda c: pl.ds(pl.multiple_of(place(c) * own, own), own)

    def turn(t, at):
        half = HEAD // 2
        t = t.astype(jnp.bfloat16).astype(jnp.float32)
        a, b, cos, sin = t[:, :half], t[:, half:], cos_s[at, :], sin_s[at, :]
        return (a * cos - b * sin).astype(jnp.bfloat16), (b * cos + a * sin).astype(jnp.bfloat16)

    def project(group, c):
        at = rows(c)
        half = HEAD // 2
        t = _dot(a_s[at, :], w_s[group], 1, 0)
        into = (kv_s, q_s)[group]
        into[at, :half], into[at, half:HEAD] = turn(t[:, :HEAD], at)
        if group == 0:
            into[at, HEAD:] = t[:, HEAD:].astype(jnp.bfloat16)
        else:
            into[at, HEAD : HEAD + half], into[at, HEAD + half :] = turn(t[:, HEAD:], at)

    to_z = (y == 0) | (zh == 0)
    from_z = (y == 0) | (zh == 1)

    def exchange(kind, c, src, k):
        return pltpu.make_async_remote_copy(src_ref=src.at[rows(c)], dst_ref=got.at[kind, rows(c)], send_sem=sem["kv"].at[0, kind, c],
                                            recv_sem=sem["kv"].at[1, kind, c], device_id=sp(k), device_id_type=MESH)

    def share_z(c):
        @pl.when(to_z)
        def _():
            exchange(1, c, kv_s, 4).start()

    def share_y(c):
        @pl.when(y == 0)
        def _():
            exchange(0, c, kv_s, 8).start()

    def forward(c):
        @pl.when(y == 0)
        def _():
            here = got.at[1, rows(c)]
            pltpu.make_async_copy(here, here, sem["kv"].at[1, 1, c]).wait()
            exchange(2, c, got.at[1], 8).start()

    def early(c, _):
        project(0, c)
        share_y(c)

    def late(c, _):
        project(0, c)
        share_z(c)
        share_y(c)

    def queries(c, _):
        project(1, c)

    def relay(i):
        arrived(slot(flip(g, 2), i, n), sem["a2"], (i,))
        send(slot(flip(g, 2), i, n), slot(flip(g, 2), i, n), sem["af"], (i,), sp(1))

    pass_y(0)
    pass_z(0)
    arrived(half(2, d), sem["o1"], (0,))
    send(half(2, d), half(2, d), sem["o1"], (2,), sp(6), inner)
    o_on(1, True)
    for i in range(ROWS):
        arrived(slot(flip(g, 1), i, n), sem["a1"], (i,))
    complete(0)
    lax.fori_loop(0, 2, early, None)
    pass_y(1)
    pass_z(1)
    arrived(half(8, d), sem["o3"], (0,))
    o_on(4)
    for i in range(ROWS):
        relay(i)

    for i, k in enumerate((6, 4)):
        pl.when(inner)(functools.partial(arrived, half(k, d), sem["o1"], (1 + i,)))
        send(half(k, d), half(k, d), sem["o1"], (3 + i,), sp(2), inner)
        o_on(k // 2, True, inner)
    share_z(0)
    share_z(1)

    for i in range(ROWS):
        arrived(slot(flip(g, 3), i, n), sem["af"], (i,))
    lax.fori_loop(2, 4, late, None)
    complete(1)
    lax.fori_loop(0, 4, queries, None)
    ones = jnp.ones((8, own), jnp.bfloat16)
    def block(keys, values, first=None):
        pieces = [(i, h) for i in range(first or 0, 4) for h in range(2)]
        scores = [_dot(keys, q_s[i * STRIP : (i + 1) * STRIP, h * HEAD : (h + 1) * HEAD], 1, 1) for i, h in pieces]
        weights, keeps = [], []
        for (i, h), sc in zip(pieces, scores):
            cols = slice((2 * i + h) * STRIP, (2 * i + h + 1) * STRIP)
            if i == first:
                sc = jnp.where(gap_s[...] >= 0, sc, HIDDEN)
            old = top_s[:, cols]
            top = jnp.maximum(old, sc.max(axis=0, keepdims=True))
            top_s[:, cols] = top
            weights.append(jnp.exp2((sc - top) * e).astype(jnp.bfloat16))
            keeps.append(jnp.exp2((old - top) * e))
        turned_values = jnp.concatenate([values.T, ones], axis=0)
        for (i, h), p, keep in zip(pieces, weights, keeps):
            cols = slice((2 * i + h) * STRIP, (2 * i + h + 1) * STRIP)
            mix_s[:, cols] = mix_s[:, cols] * keep + _dot(turned_values, p, 1, 0)

    for i in range(4):
        block(kv_s[i * own : (i + 1) * own, :HEAD], kv_s[i * own : (i + 1) * own, HEAD:], i)
    outer = jnp.logical_not(inner)
    for i, k in enumerate((4, 6)):
        pl.when(outer)(functools.partial(arrived, half(k, d), sem["o1"], (3 + i,)))
        o_on(k // 2, True, outer)
    forward(0)
    forward(1)

    def visit(t, _):
        late, kind, c = lax.div(t, 6), lax.rem(lax.div(t, 2), 3), lax.rem(t, 2)
        c = c + 2 * late
        comes = jnp.where(kind == 1, ((y == 0) & (late == 1)) | ((y == 1) & (zh == 1)), y == 1)
        wanted = jnp.where(kind == 1, zh == 1, y == 1)

        @pl.when(comes)
        def _():
            here = got.at[kind, rows(c)]
            pltpu.make_async_copy(here, here, sem["kv"].at[1, kind, c]).wait()

        @pl.when((kind == 1) & (y == 0) & (late == 1))
        def _():
            exchange(2, c, got.at[1], 8).start()

        @pl.when(wanted)
        def _():
            block(got[kind, rows(c), :HEAD], got[kind, rows(c), HEAD:])

    lax.fori_loop(0, 6, visit, None)
    for i in (5, 6, 7):
        arrived(half(EVEN[i], d), sem["o3"], (i - 4,))
        o_on(i)
    lax.fori_loop(6, 12, visit, None)

    for at in range(8):
        i, h, cols = at // 2, at % 2, slice(at * STRIP, (at + 1) * STRIP)
        out = mix_s[:HEAD, cols] * (1 / mix_s[HEAD : HEAD + 1, cols])
        out_s[i, :, h * HEAD : (h + 1) * HEAD] = out.T.astype(jnp.bfloat16)
    columns = lambda t: seen_ref.at[:, pl.ds(pl.multiple_of(t * 2 * HEAD, 2 * HEAD), 2 * HEAD)]
    for m in (2, 3, 1):
        send(out_s.at[flip(g, m)], columns(g), sem["back"], (m - 1,), sp(m))
    kept_b = keep(out_s.at[g], columns(g), sem["bl"])
    send(half(0, other), half(0, other), sem["od"], (1, 0), sp(1))
    for i in range(1, 8):
        arrived(half(EVEN[i], other), sem["ox"], (i - 1,))
        send(half(EVEN[i], other), half(EVEN[i], other), sem["od"], (1, i), sp(1))
    for i in range(8):
        arrived(half(EVEN[i] + 1, d), sem["od"], (0, i))
        arrived(half(EVEN[i] + 1, other), sem["od"], (1, i))
    for m in (1, 2, 3):
        arrived(columns(flip(g, m)), sem["back"], (m - 1,))
    kept_b.wait()
    for copy, when in sends:
        if when is None:
            copy.wait_send()
        else:
            pl.when(when)(copy.wait_send)
    for group in (0, 1):
        for i in (0, 1):
            @pl.when(d == i)
            def _():
                for m in (2, 3):
                    first_stage(2 * group + i, m).wait_send()
        for part in (2 * group, 2 * group + 1):
            first_stage(part, 1).wait_send()

    for c in range(4):
        @pl.when(to_z)
        def _():
            exchange(1, c, kv_s, 4).wait_send()

        @pl.when(y == 0)
        def _():
            exchange(0, c, kv_s, 8).wait_send()
            exchange(2, c, got.at[1], 8).wait_send()


def attended(x, gain, wq, wk, wv, wo, freq):
    own, width = x.shape
    bf16, f32 = jnp.bfloat16, jnp.float32
    vmem, hbm = pl.BlockSpec(memory_space=pltpu.VMEM), pl.BlockSpec(memory_space=pl.ANY)
    return pl.pallas_call(
        layer,
        out_shape=[jax.ShapeDtypeStruct((own, 4 * 2 * HEAD), bf16), jax.ShapeDtypeStruct((16 * wo.shape[0], wo.shape[1]), bf16)],
        in_specs=[hbm, vmem, hbm, hbm, hbm, vmem, vmem],
        out_specs=[hbm] * 2,
        scratch_shapes=[
            pltpu.VMEM((own, width), bf16),
            pltpu.VMEM((4 * own, HEAD // 2), f32),
            pltpu.VMEM((4 * own, HEAD // 2), f32),
            pltpu.VMEM((4 * own, width), bf16),
            pltpu.VMEM((2, 16 * wk.shape[0], 2 * HEAD), bf16),
            pltpu.VMEM((4 * own, 2 * HEAD), bf16),
            pltpu.VMEM((4 * own, 2 * HEAD), bf16),
            pltpu.VMEM((3, 4 * own, 2 * HEAD), bf16),
            pltpu.VMEM((1, 8 * own), f32),
            pltpu.VMEM((HEAD + 8, 8 * own), f32),
            pltpu.VMEM((4, own, 2 * HEAD), bf16),
            pltpu.VMEM((own, STRIP), jnp.int32),
            *SEMS.values(),
        ],
        compiler_params=pltpu.CompilerParams(collective_id=0, has_side_effects=True, vmem_limit_bytes=VMEM),
    )(x, gain, wq, wk, wv, wo, freq)


def out(x_ref, seen_ref, w_ref, y_ref):
    y_ref[...] = (x_ref[...].astype(jnp.float32) + _dot(seen_ref[...], w_ref[...], 1, 0)).astype(jnp.bfloat16)


def projected(x, seen, wide):
    (own, width), inner, n = x.shape, seen.shape[1], 512
    part = pl.BlockSpec((own, n), lambda j: (0, j))
    return pl.pallas_call(
        out,
        out_shape=jax.ShapeDtypeStruct((own, width), jnp.bfloat16),
        grid=(width // n,),
        in_specs=[part, pl.BlockSpec((own, inner), lambda j: (0, 0)), pl.BlockSpec((inner, n), lambda j: (0, j))],
        out_specs=part,
        cost_estimate=pl.CostEstimate(flops=2 * own * inner * width, transcendentals=0, bytes_accessed=2 * (2 * x.size + seen.size + wide.size)),
        compiler_params=pltpu.CompilerParams(vmem_limit_bytes=VMEM),
    )(x, seen, wide)


def solution(mesh):
    def step(x, gain, wq, wk, wv, wo):
        half = HEAD // 2
        freq = THETA ** (-jnp.arange(half, dtype=jnp.float32) / half)
        seen, wide = attended(x, gain, wq, wk, wv, wo, freq[None])
        return projected(x, seen, wide)

    tokens, whole = P(("dp", "sp"), None), P("sp", None)
    return jax.shard_map(
        step,
        mesh=mesh,
        in_specs=(tokens, P(None), whole, whole, whole, whole),
        out_specs=tokens,
        check_vma=False,
    )
```

```python
import functools

import jax
import jax.numpy as jnp
from jax import lax
from jax.experimental import pallas as pl
from jax.experimental.pallas import tpu as pltpu
from jax.sharding import PartitionSpec as P

NEG = -1e30
HIDDEN = 2 * NEG
LOG2E = 1.4426950408889634
VMEM = 63 * 2**20
HEAD = 256
THETA = 10000
MESH = pl.DeviceIdType.MESH


def _dot(a, b, ca, cb):
    return lax.dot_general(a, b, (((ca,), (cb,)), ((), ())), preferred_element_type=jnp.float32)


def flip(s, k):
    for bit in (1, 2, 4, 8):
        if k & bit:
            s = s + bit - 2 * bit * lax.rem(lax.div(s, bit), 2)
    return s


def meet(s, d, ks, across):
    barrier = pltpu.get_barrier_semaphore()
    for k in ks:
        pl.semaphore_signal(barrier, inc=1, device_id={"sp": flip(s, k)}, device_id_type=MESH)
    if across:
        pl.semaphore_signal(barrier, inc=1, device_id={"dp": 1 - d}, device_id_type=MESH)
    pl.semaphore_wait(barrier, len(ks) + across)


ROWS = 2
STRIP = 512
DMA = pltpu.SemaphoreType.DMA
SEMS = dict(
    xl=DMA((ROWS,)), wl=DMA((4,)), w1=DMA((2, 4, 3)), wz=DMA((2, 2)), wy=DMA((2, 2, 2)), wx=DMA((2, 2, 4)), a2=DMA((2, ROWS)), a1=DMA((2, ROWS)),
    af=DMA((2, ROWS)), kv=DMA((2, 3, 4)), o1=DMA((2, 5)), o3=DMA((2, 4)), ox=DMA((2, 7)), od=DMA((2, 2, 8)), ol=DMA, back=DMA((2, 3)),
    bl=DMA,
)


def layer(x_ref, gain_ref, wq_ref, wk_ref, wv_ref, wo_ref, freq_ref, seen_ref, wide_ref,
          x_s, cos_s, sin_s, a_s, w_s, q_s, kv_s, got, top_s, mix_s, out_s, gap_s, *sems):
    sem = dict(zip(SEMS, sems))
    s, d = lax.axis_index("sp"), lax.axis_index("dp")
    other = 1 - d
    g, zh, y = lax.rem(s, 4), lax.rem(lax.div(s, 4), 2), lax.div(s, 8)
    own = x_ref.shape[0]
    r = wk_ref.shape[0]
    e = HEAD**-0.5 * LOG2E
    sends = []

    def send(src, dst, pair, at, to, when=None):
        copy = pltpu.make_async_remote_copy(src_ref=src, dst_ref=dst, send_sem=pair.at[(0, *at)], recv_sem=pair.at[(1, *at)], device_id=to,
                                            device_id_type=MESH)
        if when is None:
            copy.start()
        else:
            pl.when(when)(copy.start)
        sends.append((copy, when))

    def arrived(dst, pair, at):
        pltpu.make_async_copy(dst, dst, pair.at[(1, *at)]).wait()

    def keep(src, dst, at):
        copy = pltpu.make_async_copy(src, dst, at)
        copy.start()
        return copy

    sp = lambda k: {"sp": flip(s, k)}
    across = {"dp": other}
    meet(s, d, (1, 2, 3, 4, 8), True)

    def head(part, g):
        if part < 2:
            return (wk_ref, wv_ref)[part].at[:, pl.ds(pl.multiple_of(g * HEAD, HEAD), HEAD)]
        return wq_ref.at[:, pl.ds(pl.multiple_of(g * 2 * HEAD + (part - 2) * HEAD, HEAD), HEAD)]

    def rows_of(part, t, n=1):
        return w_s.at[part // 2, pl.ds(pl.multiple_of(t * r, 32), n * r), pl.ds(part % 2 * HEAD, HEAD)]

    def mine(group, k):
        return w_s.at[group, pl.ds(pl.multiple_of(lax.div(flip(s, 4 * k), 4) * (4 * r), 128), 4 * r), pl.ds(pl.multiple_of(d * HEAD, HEAD), HEAD)]

    def theirs(group, k):
        return w_s.at[group, pl.ds(pl.multiple_of(lax.div(flip(s, 4 * k), 4) * (4 * r), 128), 4 * r), pl.ds(pl.multiple_of(other * HEAD, HEAD), HEAD)]

    loads = [keep(x_ref.at[pl.ds(i * (own // ROWS), own // ROWS)], x_s.at[pl.ds(i * (own // ROWS), own // ROWS)], sem["xl"].at[i]) for i in range(ROWS)]
    def first_stage(part, m):
        return pltpu.make_async_remote_copy(src_ref=head(part, flip(g, m)), dst_ref=rows_of(part, s), send_sem=sem["w1"].at[0, part, m - 1],
                                            recv_sem=sem["w1"].at[1, part, m - 1], device_id=sp(m), device_id_type=MESH)

    for group in (0, 1):
        for m in (2, 3):
            for i in (0, 1):
                @pl.when(d == i)
                def _():
                    first_stage(2 * group + i, m).start()
        for part in (2 * group, 2 * group + 1):
            first_stage(part, 1).start()
    kept = [keep(head(part, g), rows_of(part, s), sem["wl"].at[part]) for part in range(4)]
    kept_o = keep(wo_ref, wide_ref.at[pl.ds(pl.multiple_of(s * wo_ref.shape[0], 128), wo_ref.shape[0])], sem["ol"])

    n = own // ROWS
    gain = gain_ref[...].astype(jnp.float32)
    slot = lambda t, i=0, n=own: a_s.at[pl.ds(pl.multiple_of(t * own + i * n, n), n)]
    for i in range(ROWS):
        loads[i].wait()
        wide = x_s[i * n : (i + 1) * n, :].astype(jnp.float32)
        scale = lax.rsqrt(jnp.mean(wide * wide, -1, keepdims=True) + 1e-6)
        a_s[pl.ds(pl.multiple_of(g * own + i * n, n), n), :] = (wide * scale * gain).astype(jnp.bfloat16)
    gap_s[...] = lax.broadcasted_iota(jnp.int32, gap_s.shape, 1) - lax.broadcasted_iota(jnp.int32, gap_s.shape, 0)
    top_s[...] = jnp.full(top_s.shape, NEG, jnp.float32)
    mix_s[...] = jnp.zeros(mix_s.shape, jnp.float32)
    for i in range(ROWS):
        send(slot(g, i, n), slot(g, i, n), sem["a1"], (i,), sp(1))
    for copy in kept:
        copy.wait()

    def near(group, h):
        return w_s.at[group, pl.ds(pl.multiple_of(lax.div(flip(s, 2), 2) * (2 * r), 64), 2 * r), pl.ds(pl.multiple_of(h * HEAD, HEAD), HEAD)]

    def from_cluster(group):
        for part in (2 * group, 2 * group + 1):
            arrived(rows_of(part, flip(s, 1)), sem["w1"], (part, 0))
        for i in (0, 1):
            @pl.when(d == i)
            def _():
                for m in (2, 3):
                    arrived(rows_of(2 * group + i, flip(s, m)), sem["w1"], (2 * group + i, m - 1))

    def to_neighbour(i):
        send(slot(g, i, n), slot(g, i, n), sem["a2"], (i,), sp(2))

    for group in (0, 1):
        from_cluster(group)
        send(mine(group, 0), mine(group, 0), sem["wz"], (group,), sp(4))
        send(mine(group, 0), mine(group, 0), sem["wy"], (group, 0), sp(8))
        send(near(group, d), near(group, d), sem["wx"], (group, 3), across)
        if group == 0:
            for i in range(ROWS // 2):
                to_neighbour(i)

    orows, ocols = wo_ref.shape[0], wo_ref.shape[1] // 2
    half = lambda t, h: wide_ref.at[pl.ds(pl.multiple_of(flip(s, t) * orows, 128), orows), pl.ds(pl.multiple_of(h * ocols, 128), ocols)]
    EVEN = (0, 2, 4, 6, 8, 10, 12, 14)
    kept_o.wait()
    inner = lax.rem(lax.div(s, 2), 2) + zh == 1
    send(half(0, d), half(0, d), sem["o1"], (0,), sp(2))
    send(half(0, d), half(0, d), sem["o1"], (1,), sp(6), inner)
    for i in range(ROWS // 2, ROWS):
        to_neighbour(i)

    def o_on(i, to_y=False, when=None):
        k = EVEN[i]
        if to_y:
            send(half(k, d), half(k, d), sem["o3"], (i,), sp(8), when)
        if i:
            send(half(k, d), half(k, d), sem["ox"], (i - 1,), across, when)
        send(half(k, d), half(k, d), sem["od"], (0, i), sp(1), when)

    o_on(0, True)

    for i in range(4):
        spot = (lax.div(s, 4) * 4 + i) * own + lax.broadcasted_iota(jnp.int32, (own, HEAD // 2), 0)
        angle = spot.astype(jnp.float32) * freq_ref[...]
        cos_s[i * own : (i + 1) * own, :] = jnp.cos(angle)
        sin_s[i * own : (i + 1) * own, :] = jnp.sin(angle)

    def pass_y(group):
        arrived(mine(group, 2), sem["wy"], (group, 0))
        send(mine(group, 2), mine(group, 2), sem["wx"], (group, 0), across)

    def pass_z(group):
        arrived(mine(group, 1), sem["wz"], (group,))
        send(mine(group, 1), mine(group, 1), sem["wy"], (group, 1), sp(8))
        send(mine(group, 1), mine(group, 1), sem["wx"], (group, 1), across)
        arrived(mine(group, 3), sem["wy"], (group, 1))
        send(mine(group, 3), mine(group, 3), sem["wx"], (group, 2), across)

    def complete(group):
        for i, k in enumerate((2, 1, 3)):
            arrived(theirs(group, k), sem["wx"], (group, i))
        arrived(near(group, other), sem["wx"], (group, 3))

    place = lambda c: lax.rem(lax.div(g, 2) * 2 + c, 4)
    rows = lambda c: pl.ds(pl.multiple_of(place(c) * own, own), own)

    def turn(t, at):
        half = HEAD // 2
        t = t.astype(jnp.bfloat16).astype(jnp.float32)
        a, b, cos, sin = t[:, :half], t[:, half:], cos_s[at, :], sin_s[at, :]
        return (a * cos - b * sin).astype(jnp.bfloat16), (b * cos + a * sin).astype(jnp.bfloat16)

    def project(group, c):
        at = rows(c)
        half = HEAD // 2
        t = _dot(a_s[at, :], w_s[group], 1, 0)
        into = (kv_s, q_s)[group]
        into[at, :half], into[at, half:HEAD] = turn(t[:, :HEAD], at)
        if group == 0:
            into[at, HEAD:] = t[:, HEAD:].astype(jnp.bfloat16)
        else:
            into[at, HEAD : HEAD + half], into[at, HEAD + half :] = turn(t[:, HEAD:], at)

    to_z = (y == 0) | (zh == 0)
    from_z = (y == 0) | (zh == 1)

    def exchange(kind, c, src, k):
        return pltpu.make_async_remote_copy(src_ref=src.at[rows(c)], dst_ref=got.at[kind, rows(c)], send_sem=sem["kv"].at[0, kind, c],
                                            recv_sem=sem["kv"].at[1, kind, c], device_id=sp(k), device_id_type=MESH)

    def share_z(c):
        @pl.when(to_z)
        def _():
            exchange(1, c, kv_s, 4).start()

    def share_y(c):
        @pl.when(y == 0)
        def _():
            exchange(0, c, kv_s, 8).start()

    def forward(c):
        @pl.when(y == 0)
        def _():
            here = got.at[1, rows(c)]
            pltpu.make_async_copy(here, here, sem["kv"].at[1, 1, c]).wait()
            exchange(2, c, got.at[1], 8).start()

    def early(c, _):
        project(0, c)
        share_y(c)

    def late(c, _):
        project(0, c)
        share_z(c)
        share_y(c)

    def queries(c, _):
        project(1, c)

    def relay(i):
        arrived(slot(flip(g, 2), i, n), sem["a2"], (i,))
        send(slot(flip(g, 2), i, n), slot(flip(g, 2), i, n), sem["af"], (i,), sp(1))

    pass_y(0)
    pass_z(0)
    arrived(half(2, d), sem["o1"], (0,))
    send(half(2, d), half(2, d), sem["o1"], (2,), sp(6), inner)
    o_on(1, True)
    for i in range(ROWS):
        arrived(slot(flip(g, 1), i, n), sem["a1"], (i,))
    complete(0)
    lax.fori_loop(0, 2, early, None)
    pass_y(1)
    pass_z(1)
    arrived(half(8, d), sem["o3"], (0,))
    o_on(4)
    for i in range(ROWS):
        relay(i)

    for i, k in enumerate((6, 4)):
        pl.when(inner)(functools.partial(arrived, half(k, d), sem["o1"], (1 + i,)))
        send(half(k, d), half(k, d), sem["o1"], (3 + i,), sp(2), inner)
        o_on(k // 2, True, inner)
    share_z(0)
    share_z(1)

    for i in range(ROWS):
        arrived(slot(flip(g, 3), i, n), sem["af"], (i,))
    lax.fori_loop(2, 4, late, None)
    complete(1)
    lax.fori_loop(0, 4, queries, None)
    ones = jnp.ones((8, own), jnp.bfloat16)
    def block(keys, values, first=None):
        pieces = [(i, h) for i in range(first or 0, 4) for h in range(2)]
        scores = [_dot(keys, q_s[i * STRIP : (i + 1) * STRIP, h * HEAD : (h + 1) * HEAD], 1, 1) for i, h in pieces]
        weights, keeps = [], []
        for (i, h), sc in zip(pieces, scores):
            cols = slice((2 * i + h) * STRIP, (2 * i + h + 1) * STRIP)
            if i == first:
                sc = jnp.where(gap_s[...] >= 0, sc, HIDDEN)
            old = top_s[:, cols]
            top = jnp.maximum(old, sc.max(axis=0, keepdims=True))
            top_s[:, cols] = top
            weights.append(jnp.exp2((sc - top) * e).astype(jnp.bfloat16))
            keeps.append(jnp.exp2((old - top) * e))
        turned_values = jnp.concatenate([values.T, ones], axis=0)
        for (i, h), p, keep in zip(pieces, weights, keeps):
            cols = slice((2 * i + h) * STRIP, (2 * i + h + 1) * STRIP)
            mix_s[:, cols] = mix_s[:, cols] * keep + _dot(turned_values, p, 1, 0)

    for i in range(4):
        block(kv_s[i * own : (i + 1) * own, :HEAD], kv_s[i * own : (i + 1) * own, HEAD:], i)
    outer = jnp.logical_not(inner)
    for i, k in enumerate((4, 6)):
        pl.when(outer)(functools.partial(arrived, half(k, d), sem["o1"], (3 + i,)))
        o_on(k // 2, True, outer)
    forward(0)
    forward(1)

    def visit(t, _):
        late, kind, c = lax.div(t, 6), lax.rem(lax.div(t, 2), 3), lax.rem(t, 2)
        c = c + 2 * late
        comes = jnp.where(kind == 1, ((y == 0) & (late == 1)) | ((y == 1) & (zh == 1)), y == 1)
        wanted = jnp.where(kind == 1, zh == 1, y == 1)

        @pl.when(comes)
        def _():
            here = got.at[kind, rows(c)]
            pltpu.make_async_copy(here, here, sem["kv"].at[1, kind, c]).wait()

        @pl.when((kind == 1) & (y == 0) & (late == 1))
        def _():
            exchange(2, c, got.at[1], 8).start()

        @pl.when(wanted)
        def _():
            block(got[kind, rows(c), :HEAD], got[kind, rows(c), HEAD:])

    lax.fori_loop(0, 6, visit, None)
    for i in (5, 6, 7):
        arrived(half(EVEN[i], d), sem["o3"], (i - 4,))
        o_on(i)
    lax.fori_loop(6, 12, visit, None)

    for at in range(8):
        i, h, cols = at // 2, at % 2, slice(at * STRIP, (at + 1) * STRIP)
        out = mix_s[:HEAD, cols] * (1 / mix_s[HEAD : HEAD + 1, cols])
        out_s[i, :, h * HEAD : (h + 1) * HEAD] = out.T.astype(jnp.bfloat16)
    columns = lambda t: seen_ref.at[:, pl.ds(pl.multiple_of(t * 2 * HEAD, 2 * HEAD), 2 * HEAD)]
    for m in (2, 3, 1):
        send(out_s.at[flip(g, m)], columns(g), sem["back"], (m - 1,), sp(m))
    kept_b = keep(out_s.at[g], columns(g), sem["bl"])
    send(half(0, other), half(0, other), sem["od"], (1, 0), sp(1))
    for i in range(1, 8):
        arrived(half(EVEN[i], other), sem["ox"], (i - 1,))
        send(half(EVEN[i], other), half(EVEN[i], other), sem["od"], (1, i), sp(1))
    for i in range(8):
        arrived(half(EVEN[i] + 1, d), sem["od"], (0, i))
        arrived(half(EVEN[i] + 1, other), sem["od"], (1, i))
    for m in (1, 2, 3):
        arrived(columns(flip(g, m)), sem["back"], (m - 1,))
    kept_b.wait()
    for copy, when in sends:
        if when is None:
            copy.wait_send()
        else:
            pl.when(when)(copy.wait_send)
    for group in (0, 1):
        for i in (0, 1):
            @pl.when(d == i)
            def _():
                for m in (2, 3):
                    first_stage(2 * group + i, m).wait_send()
        for part in (2 * group, 2 * group + 1):
            first_stage(part, 1).wait_send()

    for c in range(4):
        @pl.when(to_z)
        def _():
            exchange(1, c, kv_s, 4).wait_send()

        @pl.when(y == 0)
        def _():
            exchange(0, c, kv_s, 8).wait_send()
            exchange(2, c, got.at[1], 8).wait_send()


def attended(x, gain, wq, wk, wv, wo, freq):
    own, width = x.shape
    bf16, f32 = jnp.bfloat16, jnp.float32
    vmem, hbm = pl.BlockSpec(memory_space=pltpu.VMEM), pl.BlockSpec(memory_space=pl.ANY)
    return pl.pallas_call(
        layer,
        out_shape=[jax.ShapeDtypeStruct((own, 4 * 2 * HEAD), bf16), jax.ShapeDtypeStruct((16 * wo.shape[0], wo.shape[1]), bf16)],
        in_specs=[hbm, vmem, hbm, hbm, hbm, vmem, vmem],
        out_specs=[hbm] * 2,
        scratch_shapes=[
            pltpu.VMEM((own, width), bf16),
            pltpu.VMEM((4 * own, HEAD // 2), f32),
            pltpu.VMEM((4 * own, HEAD // 2), f32),
            pltpu.VMEM((4 * own, width), bf16),
            pltpu.VMEM((2, 16 * wk.shape[0], 2 * HEAD), bf16),
            pltpu.VMEM((4 * own, 2 * HEAD), bf16),
            pltpu.VMEM((4 * own, 2 * HEAD), bf16),
            pltpu.VMEM((3, 4 * own, 2 * HEAD), bf16),
            pltpu.VMEM((1, 8 * own), f32),
            pltpu.VMEM((HEAD + 8, 8 * own), f32),
            pltpu.VMEM((4, own, 2 * HEAD), bf16),
            pltpu.VMEM((own, STRIP), jnp.int32),
            *SEMS.values(),
        ],
        compiler_params=pltpu.CompilerParams(collective_id=0, has_side_effects=True, vmem_limit_bytes=VMEM),
    )(x, gain, wq, wk, wv, wo, freq)


def solution(mesh):
    def step(x, gain, wq, wk, wv, wo):
        half = HEAD // 2
        freq = THETA ** (-jnp.arange(half, dtype=jnp.float32) / half)
        seen, wide = attended(x, gain, wq, wk, wv, wo, freq[None])
        y = jnp.dot(seen, wide, preferred_element_type=jnp.float32)
        return (x.astype(jnp.float32) + y).astype(jnp.bfloat16)

    tokens, whole = P(("dp", "sp"), None), P("sp", None)
    return jax.shard_map(
        step,
        mesh=mesh,
        in_specs=(tokens, P(None), whole, whole, whole, whole),
        out_specs=tokens,
        check_vma=False,
    )
```

```python
import functools

import jax
import jax.numpy as jnp
from jax import lax
from jax.experimental import pallas as pl
from jax.experimental.pallas import tpu as pltpu
from jax.sharding import PartitionSpec as P

NEG = -1e30
HIDDEN = 2 * NEG
LOG2E = 1.4426950408889634
VMEM = 63 * 2**20
HEAD = 256
THETA = 10000
MESH = pl.DeviceIdType.MESH


def _dot(a, b, ca, cb):
    return lax.dot_general(a, b, (((ca,), (cb,)), ((), ())), preferred_element_type=jnp.float32)


def flip(s, k):
    for bit in (1, 2, 4, 8):
        if k & bit:
            s = s + bit - 2 * bit * lax.rem(lax.div(s, bit), 2)
    return s


def meet(s, d, ks, across):
    barrier = pltpu.get_barrier_semaphore()
    for k in ks:
        pl.semaphore_signal(barrier, inc=1, device_id={"sp": flip(s, k)}, device_id_type=MESH)
    if across:
        pl.semaphore_signal(barrier, inc=1, device_id={"dp": 1 - d}, device_id_type=MESH)
    pl.semaphore_wait(barrier, len(ks) + across)


ROWS = 2
STRIP = 512
DMA = pltpu.SemaphoreType.DMA
SEMS = dict(
    xl=DMA((ROWS,)), wl=DMA((4,)), w1=DMA((2, 4, 3)), wz=DMA((2, 2)), wy=DMA((2, 2, 2)), wx=DMA((2, 2, 4)), a2=DMA((2, ROWS)), a1=DMA((2, ROWS)),
    af=DMA((2, ROWS)), kv=DMA((2, 3, 4)), o1=DMA((2, 5)), o3=DMA((2, 4)), ox=DMA((2, 7)), od=DMA((2, 2, 8)), ol=DMA, back=DMA((2, 3)),
    bl=DMA,
)


def layer(x_ref, gain_ref, wq_ref, wk_ref, wv_ref, wo_ref, freq_ref, seen_ref, wide_ref,
          x_s, cos_s, sin_s, a_s, w_s, q_s, kv_s, got, top_s, mix_s, out_s, gap_s, *sems):
    sem = dict(zip(SEMS, sems))
    s, d = lax.axis_index("sp"), lax.axis_index("dp")
    other = 1 - d
    g, zh, y = lax.rem(s, 4), lax.rem(lax.div(s, 4), 2), lax.div(s, 8)
    own = x_ref.shape[0]
    r = wk_ref.shape[0]
    e = HEAD**-0.5 * LOG2E
    sends = []

    def send(src, dst, pair, at, to, when=None):
        copy = pltpu.make_async_remote_copy(src_ref=src, dst_ref=dst, send_sem=pair.at[(0, *at)], recv_sem=pair.at[(1, *at)], device_id=to,
                                            device_id_type=MESH)
        if when is None:
            copy.start()
        else:
            pl.when(when)(copy.start)
        sends.append((copy, when))

    def arrived(dst, pair, at):
        pltpu.make_async_copy(dst, dst, pair.at[(1, *at)]).wait()

    def keep(src, dst, at):
        copy = pltpu.make_async_copy(src, dst, at)
        copy.start()
        return copy

    sp = lambda k: {"sp": flip(s, k)}
    across = {"dp": other}
    meet(s, d, (1, 2, 3, 4, 8), True)

    def head(part, g):
        if part < 2:
            return (wk_ref, wv_ref)[part].at[:, pl.ds(pl.multiple_of(g * HEAD, HEAD), HEAD)]
        return wq_ref.at[:, pl.ds(pl.multiple_of(g * 2 * HEAD + (part - 2) * HEAD, HEAD), HEAD)]

    def rows_of(part, t, n=1):
        return w_s.at[part // 2, pl.ds(pl.multiple_of(t * r, 32), n * r), pl.ds(part % 2 * HEAD, HEAD)]

    def mine(group, k):
        return w_s.at[group, pl.ds(pl.multiple_of(lax.div(flip(s, 4 * k), 4) * (4 * r), 128), 4 * r), pl.ds(pl.multiple_of(d * HEAD, HEAD), HEAD)]

    def theirs(group, k):
        return w_s.at[group, pl.ds(pl.multiple_of(lax.div(flip(s, 4 * k), 4) * (4 * r), 128), 4 * r), pl.ds(pl.multiple_of(other * HEAD, HEAD), HEAD)]

    loads = [keep(x_ref.at[pl.ds(i * (own // ROWS), own // ROWS)], x_s.at[pl.ds(i * (own // ROWS), own // ROWS)], sem["xl"].at[i]) for i in range(ROWS)]
    def first_stage(part, m):
        return pltpu.make_async_remote_copy(src_ref=head(part, flip(g, m)), dst_ref=rows_of(part, s), send_sem=sem["w1"].at[0, part, m - 1],
                                            recv_sem=sem["w1"].at[1, part, m - 1], device_id=sp(m), device_id_type=MESH)

    for group in (0, 1):
        for m in (2, 3):
            for i in (0, 1):
                @pl.when(d == i)
                def _():
                    first_stage(2 * group + i, m).start()
        for part in (2 * group, 2 * group + 1):
            first_stage(part, 1).start()
    kept = [keep(head(part, g), rows_of(part, s), sem["wl"].at[part]) for part in range(4)]
    kept_o = keep(wo_ref, wide_ref.at[pl.ds(pl.multiple_of(s * wo_ref.shape[0], 128), wo_ref.shape[0])], sem["ol"])

    n = own // ROWS
    gain = gain_ref[...].astype(jnp.float32)
    slot = lambda t, i=0, n=own: a_s.at[pl.ds(pl.multiple_of(t * own + i * n, n), n)]
    for i in range(ROWS):
        loads[i].wait()
        wide = x_s[i * n : (i + 1) * n, :].astype(jnp.float32)
        scale = lax.rsqrt(jnp.mean(wide * wide, -1, keepdims=True) + 1e-6)
        a_s[pl.ds(pl.multiple_of(g * own + i * n, n), n), :] = (wide * scale * gain).astype(jnp.bfloat16)
    gap_s[...] = lax.broadcasted_iota(jnp.int32, gap_s.shape, 1) - lax.broadcasted_iota(jnp.int32, gap_s.shape, 0)
    top_s[...] = jnp.full(top_s.shape, NEG, jnp.float32)
    mix_s[...] = jnp.zeros(mix_s.shape, jnp.float32)
    for i in range(ROWS):
        send(slot(g, i, n), slot(g, i, n), sem["a1"], (i,), sp(1))
    for copy in kept:
        copy.wait()

    def near(group, h):
        return w_s.at[group, pl.ds(pl.multiple_of(lax.div(flip(s, 2), 2) * (2 * r), 64), 2 * r), pl.ds(pl.multiple_of(h * HEAD, HEAD), HEAD)]

    def from_cluster(group):
        for part in (2 * group, 2 * group + 1):
            arrived(rows_of(part, flip(s, 1)), sem["w1"], (part, 0))
        for i in (0, 1):
            @pl.when(d == i)
            def _():
                for m in (2, 3):
                    arrived(rows_of(2 * group + i, flip(s, m)), sem["w1"], (2 * group + i, m - 1))

    def to_neighbour(i):
        send(slot(g, i, n), slot(g, i, n), sem["a2"], (i,), sp(2))

    for group in (0, 1):
        from_cluster(group)
        send(mine(group, 0), mine(group, 0), sem["wz"], (group,), sp(4))
        send(mine(group, 0), mine(group, 0), sem["wy"], (group, 0), sp(8))
        send(near(group, d), near(group, d), sem["wx"], (group, 3), across)
        if group == 0:
            for i in range(ROWS // 2):
                to_neighbour(i)

    orows, ocols = wo_ref.shape[0], wo_ref.shape[1] // 2
    half = lambda t, h: wide_ref.at[pl.ds(pl.multiple_of(flip(s, t) * orows, 128), orows), pl.ds(pl.multiple_of(h * ocols, 128), ocols)]
    EVEN = (0, 2, 4, 6, 8, 10, 12, 14)
    kept_o.wait()
    inner = lax.rem(lax.div(s, 2), 2) + zh == 1
    send(half(0, d), half(0, d), sem["o1"], (0,), sp(2))
    send(half(0, d), half(0, d), sem["o1"], (1,), sp(6), inner)
    for i in range(ROWS // 2, ROWS):
        to_neighbour(i)

    def o_on(i, to_y=False, when=None):
        k = EVEN[i]
        if to_y:
            send(half(k, d), half(k, d), sem["o3"], (i,), sp(8), when)
        if i:
            send(half(k, d), half(k, d), sem["ox"], (i - 1,), across, when)
        send(half(k, d), half(k, d), sem["od"], (0, i), sp(1), when)

    o_on(0, True)

    for i in range(4):
        spot = (lax.div(s, 4) * 4 + i) * own + lax.broadcasted_iota(jnp.int32, (own, HEAD // 2), 0)
        angle = spot.astype(jnp.float32) * freq_ref[...]
        cos_s[i * own : (i + 1) * own, :] = jnp.cos(angle)
        sin_s[i * own : (i + 1) * own, :] = jnp.sin(angle)

    def pass_y(group):
        arrived(mine(group, 2), sem["wy"], (group, 0))
        send(mine(group, 2), mine(group, 2), sem["wx"], (group, 0), across)

    def pass_z(group):
        arrived(mine(group, 1), sem["wz"], (group,))
        send(mine(group, 1), mine(group, 1), sem["wy"], (group, 1), sp(8))
        send(mine(group, 1), mine(group, 1), sem["wx"], (group, 1), across)

    def pass_last(group):
        arrived(mine(group, 3), sem["wy"], (group, 1))
        send(mine(group, 3), mine(group, 3), sem["wx"], (group, 2), across)

    def complete(group):
        for i, k in enumerate((2, 1, 3)):
            arrived(theirs(group, k), sem["wx"], (group, i))
        arrived(near(group, other), sem["wx"], (group, 3))

    place = lambda c: lax.rem(lax.div(g, 2) * 2 + c, 4)
    rows = lambda c: pl.ds(pl.multiple_of(place(c) * own, own), own)

    def turn(t, at):
        half = HEAD // 2
        t = t.astype(jnp.bfloat16).astype(jnp.float32)
        a, b, cos, sin = t[:, :half], t[:, half:], cos_s[at, :], sin_s[at, :]
        return (a * cos - b * sin).astype(jnp.bfloat16), (b * cos + a * sin).astype(jnp.bfloat16)

    def project(group, c):
        at = rows(c)
        half = HEAD // 2
        t = _dot(a_s[at, :], w_s[group], 1, 0)
        into = (kv_s, q_s)[group]
        into[at, :half], into[at, half:HEAD] = turn(t[:, :HEAD], at)
        if group == 0:
            into[at, HEAD:] = t[:, HEAD:].astype(jnp.bfloat16)
        else:
            into[at, HEAD : HEAD + half], into[at, HEAD + half :] = turn(t[:, HEAD:], at)

    to_z = (y == 0) | (zh == 0)
    from_z = (y == 0) | (zh == 1)

    def exchange(kind, c, src, k):
        return pltpu.make_async_remote_copy(src_ref=src.at[rows(c)], dst_ref=got.at[kind, rows(c)], send_sem=sem["kv"].at[0, kind, c],
                                            recv_sem=sem["kv"].at[1, kind, c], device_id=sp(k), device_id_type=MESH)

    def share_z(c):
        @pl.when(to_z)
        def _():
            exchange(1, c, kv_s, 4).start()

    def share_y(c):
        @pl.when(y == 0)
        def _():
            exchange(0, c, kv_s, 8).start()

    def forward(c):
        @pl.when(y == 0)
        def _():
            here = got.at[1, rows(c)]
            pltpu.make_async_copy(here, here, sem["kv"].at[1, 1, c]).wait()
            exchange(2, c, got.at[1], 8).start()

    def early(c, _):
        project(0, c)
        share_y(c)

    def late(c, _):
        project(0, c)
        share_z(c)
        share_y(c)

    def queries(c, _):
        project(1, c)

    def relay(i):
        arrived(slot(flip(g, 2), i, n), sem["a2"], (i,))
        send(slot(flip(g, 2), i, n), slot(flip(g, 2), i, n), sem["af"], (i,), sp(1))

    pass_y(0)
    pass_z(0)
    pass_last(0)
    arrived(half(2, d), sem["o1"], (0,))
    send(half(2, d), half(2, d), sem["o1"], (2,), sp(6), inner)
    o_on(1, True)
    for i in range(ROWS):
        arrived(slot(flip(g, 1), i, n), sem["a1"], (i,))
    complete(0)
    lax.fori_loop(0, 2, early, None)
    relay(0)
    pass_y(1)
    pass_z(1)
    arrived(half(8, d), sem["o3"], (0,))
    o_on(4)
    relay(1)

    for i, k in enumerate((6, 4)):
        pl.when(inner)(functools.partial(arrived, half(k, d), sem["o1"], (1 + i,)))
        send(half(k, d), half(k, d), sem["o1"], (3 + i,), sp(2), inner)
        o_on(k // 2, True, inner)
    share_z(0)
    share_z(1)

    for i in range(ROWS):
        arrived(slot(flip(g, 3), i, n), sem["af"], (i,))
    lax.fori_loop(2, 4, late, None)
    pass_last(1)
    complete(1)
    lax.fori_loop(0, 4, queries, None)
    ones = jnp.ones((8, own), jnp.bfloat16)
    def block(keys, values, first=None):
        pieces = [(i, h) for i in range(first or 0, 4) for h in range(2)]
        scores = [_dot(keys, q_s[i * STRIP : (i + 1) * STRIP, h * HEAD : (h + 1) * HEAD], 1, 1) for i, h in pieces]
        weights, keeps = [], []
        for (i, h), sc in zip(pieces, scores):
            cols = slice((2 * i + h) * STRIP, (2 * i + h + 1) * STRIP)
            if i == first:
                sc = jnp.where(gap_s[...] >= 0, sc, HIDDEN)
            old = top_s[:, cols]
            top = jnp.maximum(old, sc.max(axis=0, keepdims=True))
            top_s[:, cols] = top
            weights.append(jnp.exp2((sc - top) * e).astype(jnp.bfloat16))
            keeps.append(jnp.exp2((old - top) * e))
        turned_values = jnp.concatenate([values.T, ones], axis=0)
        for (i, h), p, keep in zip(pieces, weights, keeps):
            cols = slice((2 * i + h) * STRIP, (2 * i + h + 1) * STRIP)
            mix_s[:, cols] = mix_s[:, cols] * keep + _dot(turned_values, p, 1, 0)

    for i in range(4):
        block(kv_s[i * own : (i + 1) * own, :HEAD], kv_s[i * own : (i + 1) * own, HEAD:], i)
    outer = jnp.logical_not(inner)
    for i, k in enumerate((4, 6)):
        pl.when(outer)(functools.partial(arrived, half(k, d), sem["o1"], (3 + i,)))
        o_on(k // 2, True, outer)
    forward(0)
    forward(1)

    def visit(t, _):
        late, kind, c = lax.div(t, 6), lax.rem(lax.div(t, 2), 3), lax.rem(t, 2)
        c = c + 2 * late
        comes = jnp.where(kind == 1, ((y == 0) & (late == 1)) | ((y == 1) & (zh == 1)), y == 1)
        wanted = jnp.where(kind == 1, zh == 1, y == 1)

        @pl.when(comes)
        def _():
            here = got.at[kind, rows(c)]
            pltpu.make_async_copy(here, here, sem["kv"].at[1, kind, c]).wait()

        @pl.when((kind == 1) & (y == 0) & (late == 1))
        def _():
            exchange(2, c, got.at[1], 8).start()

        @pl.when(wanted)
        def _():
            block(got[kind, rows(c), :HEAD], got[kind, rows(c), HEAD:])

    lax.fori_loop(0, 6, visit, None)
    for i in (5, 6, 7):
        arrived(half(EVEN[i], d), sem["o3"], (i - 4,))
        o_on(i)
    lax.fori_loop(6, 12, visit, None)

    for at in range(8):
        i, h, cols = at // 2, at % 2, slice(at * STRIP, (at + 1) * STRIP)
        out = mix_s[:HEAD, cols] * (1 / mix_s[HEAD : HEAD + 1, cols])
        out_s[i, :, h * HEAD : (h + 1) * HEAD] = out.T.astype(jnp.bfloat16)
    columns = lambda t: seen_ref.at[:, pl.ds(pl.multiple_of(t * 2 * HEAD, 2 * HEAD), 2 * HEAD)]
    for m in (2, 3, 1):
        send(out_s.at[flip(g, m)], columns(g), sem["back"], (m - 1,), sp(m))
    kept_b = keep(out_s.at[g], columns(g), sem["bl"])
    send(half(0, other), half(0, other), sem["od"], (1, 0), sp(1))
    for i in range(1, 8):
        arrived(half(EVEN[i], other), sem["ox"], (i - 1,))
        send(half(EVEN[i], other), half(EVEN[i], other), sem["od"], (1, i), sp(1))
    for i in range(8):
        arrived(half(EVEN[i] + 1, d), sem["od"], (0, i))
        arrived(half(EVEN[i] + 1, other), sem["od"], (1, i))
    for m in (1, 2, 3):
        arrived(columns(flip(g, m)), sem["back"], (m - 1,))
    kept_b.wait()
    for copy, when in sends:
        if when is None:
            copy.wait_send()
        else:
            pl.when(when)(copy.wait_send)
    for group in (0, 1):
        for i in (0, 1):
            @pl.when(d == i)
            def _():
                for m in (2, 3):
                    first_stage(2 * group + i, m).wait_send()
        for part in (2 * group, 2 * group + 1):
            first_stage(part, 1).wait_send()

    for c in range(4):
        @pl.when(to_z)
        def _():
            exchange(1, c, kv_s, 4).wait_send()

        @pl.when(y == 0)
        def _():
            exchange(0, c, kv_s, 8).wait_send()
            exchange(2, c, got.at[1], 8).wait_send()


def attended(x, gain, wq, wk, wv, wo, freq):
    own, width = x.shape
    bf16, f32 = jnp.bfloat16, jnp.float32
    vmem, hbm = pl.BlockSpec(memory_space=pltpu.VMEM), pl.BlockSpec(memory_space=pl.ANY)
    return pl.pallas_call(
        layer,
        out_shape=[jax.ShapeDtypeStruct((own, 4 * 2 * HEAD), bf16), jax.ShapeDtypeStruct((16 * wo.shape[0], wo.shape[1]), bf16)],
        in_specs=[hbm, vmem, hbm, hbm, hbm, vmem, vmem],
        out_specs=[hbm] * 2,
        scratch_shapes=[
            pltpu.VMEM((own, width), bf16),
            pltpu.VMEM((4 * own, HEAD // 2), f32),
            pltpu.VMEM((4 * own, HEAD // 2), f32),
            pltpu.VMEM((4 * own, width), bf16),
            pltpu.VMEM((2, 16 * wk.shape[0], 2 * HEAD), bf16),
            pltpu.VMEM((4 * own, 2 * HEAD), bf16),
            pltpu.VMEM((4 * own, 2 * HEAD), bf16),
            pltpu.VMEM((3, 4 * own, 2 * HEAD), bf16),
            pltpu.VMEM((1, 8 * own), f32),
            pltpu.VMEM((HEAD + 8, 8 * own), f32),
            pltpu.VMEM((4, own, 2 * HEAD), bf16),
            pltpu.VMEM((own, STRIP), jnp.int32),
            *SEMS.values(),
        ],
        compiler_params=pltpu.CompilerParams(collective_id=0, has_side_effects=True, vmem_limit_bytes=VMEM),
    )(x, gain, wq, wk, wv, wo, freq)


def solution(mesh):
    def step(x, gain, wq, wk, wv, wo):
        half = HEAD // 2
        freq = THETA ** (-jnp.arange(half, dtype=jnp.float32) / half)
        seen, wide = attended(x, gain, wq, wk, wv, wo, freq[None])
        y = jnp.dot(seen, wide, preferred_element_type=jnp.float32)
        return (x.astype(jnp.float32) + y).astype(jnp.bfloat16)

    tokens, whole = P(("dp", "sp"), None), P("sp", None)
    return jax.shard_map(
        step,
        mesh=mesh,
        in_specs=(tokens, P(None), whole, whole, whole, whole),
        out_specs=tokens,
        check_vma=False,
    )
```
